8 devices in a mesh: rep: 2 (over y, z), dp: 4 (over x, core).
Axes of the slice: x: 2, y: 2, z: 1, core: 2. Of those that a mesh axis runs over, the one named last changes fastest.
Arguments:
- x: bfloat16 [8, 2048, 768], P(('rep', 'dp')), parts along dimension 0
- dy: bfloat16 [8, 2048, 768], P(('rep', 'dp')), parts along dimension 0
- w_gate: bfloat16 [2, 768, 6144], replicated
- w_up: bfloat16 [2, 768, 6144], replicated
- w_down: bfloat16 [2, 6144, 768], replicated
- m_w_gate: float32 [2, 768, 6144], replicated
- m_w_up: float32 [2, 768, 6144], replicated
- m_w_down: float32 [2, 6144, 768], replicated
- v_w_gate: float32 [2, 768, 6144], replicated
- v_w_up: float32 [2, 768, 6144], replicated
- v_w_down: float32 [2, 6144, 768], replicated
Outputs:
- output 1: bfloat16 [4, 768, 6144], P('rep'), parts along dimension 0
- output 2: bfloat16 [4, 768, 6144], P('rep'), parts along dimension 0
- output 3: bfloat16 [4, 6144, 768], P('rep'), parts along dimension 0
- output 4: float32 [4, 768, 6144], P('rep'), parts along dimension 0
- output 5: float32 [4, 768, 6144], P('rep'), parts along dimension 0
- output 6: float32 [4, 6144, 768], P('rep'), parts along dimension 0
- output 7: float32 [4, 768, 6144], P('rep'), parts along dimension 0
- output 8: float32 [4, 768, 6144], P('rep'), parts along dimension 0
- output 9: float32 [4, 6144, 768], P('rep'), parts along dimension 0
There are 2 independent parts. The reference program is written for one: setup_inputs(seed, part) draws one part's arguments, and reference() takes and returns one part's arrays. A program takes and returns all parts, laid end to end along the dimension named above; an argument that names none is the same for every part.
All inputs are finite; a program needn't handle non-finite values.
Results may differ from the reference program's by a relative error of at most 0.0246.
Values are sent between devices in bfloat16 or wider.
A program may use at most 3 GiB of HBM per device.

```python
import jax
import jax.numpy as jnp
from jax import lax

SEQUENCES = 4
TOKENS = 2048
D = 768
FF = 6144
LAYERS = 2
NAMES = ("w_gate", "w_up", "w_down")
SHAPES = {"w_gate": (LAYERS, D, FF), "w_up": (LAYERS, D, FF), "w_down": (LAYERS, FF, D)}


def bump(key, n, height):
    away = (jnp.arange(n, dtype=jnp.int32) - jax.random.randint(key, (), 0, n, jnp.int32)) % n
    return jnp.where(away < n // 8, height, 1.0)


def together(key, own, strength):
    shared = jax.random.normal(key, own.shape[1:], jnp.float32)
    return (own + strength * shared) * lax.rsqrt(1 + strength * strength)


def setup_inputs(seed: int = 0, part: int = 0) -> dict:
    kx, kdy, ka, kb, kz, kf, kh, kl, *keys = jax.random.split(jax.random.key(seed), 8 + 3 * len(NAMES))
    kx, kdy, ka, kb = (jax.random.fold_in(k, part) for k in (kx, kdy, ka, kb))
    kw, km, kv = (keys[i::3] for i in range(3))
    shape = (SEQUENCES, TOKENS, D)
    much_x, much_dy = jax.random.uniform(kz, (2,), jnp.float32, 0.0, 1.0)
    loud = 2.0 ** jax.random.uniform(jax.random.fold_in(kz, 1), (), jnp.float32, -1.0, 2.0)
    layers = 2.0 ** jax.random.uniform(kl, (LAYERS, 1, 1), jnp.float32, -1.0, 1.0)
    x = together(ka, jax.random.normal(kx, shape, jnp.float32), much_x) * bump(kf, D, 4.0)
    dy = together(kb, jax.random.normal(kdy, shape, jnp.float32), much_dy)
    drawn = {"x": x.astype(jnp.bfloat16), "dy": (loud * dy * (SEQUENCES * TOKENS) ** -0.5).astype(jnp.bfloat16)}
    for key, name in zip(kw, NAMES, strict=True):
        w = jax.random.normal(key, SHAPES[name], jnp.float32) * SHAPES[name][1] ** -0.5
        drawn[name] = (w * {"w_gate": 1.0, "w_up": bump(kh, FF, 4.0), "w_down": layers}[name]).astype(jnp.bfloat16)
    for key, name in zip(km, NAMES, strict=True):
        drawn[f"m_{name}"] = 0.1 * jax.random.normal(key, SHAPES[name], jnp.float32)
    for key, name in zip(kv, NAMES, strict=True):
        drawn[f"v_{name}"] = jax.random.uniform(key, SHAPES[name], jnp.float32, 0.005, 0.015)
    return drawn


def matmul(a, w):
    return jnp.dot(a, w, preferred_element_type=jnp.float32).astype(jnp.bfloat16)


def normed(h):
    wide = h.astype(jnp.float32)
    scale = lax.rsqrt(jnp.mean(wide**2, -1, keepdims=True) + 1e-6)
    return (wide * scale).astype(jnp.bfloat16)


def layer(h, w):
    a = normed(h)
    gate = jnp.dot(a, w["w_gate"], preferred_element_type=jnp.float32)
    up = jnp.dot(a, w["w_up"], preferred_element_type=jnp.float32)
    return h + matmul((jax.nn.silu(gate) * up).astype(jnp.bfloat16), w["w_down"])


def adamw(w, m, v, g):
    m = 0.9 * m + 0.1 * g
    v = 0.95 * v + 0.05 * g * g
    step = m * lax.rsqrt(v + 1e-8) + 0.1 * w
    return (w - 0.02 * step).astype(jnp.bfloat16), m, v


def stack(weights, h):
    return lax.scan(lambda h, w: (layer(h, w), None), h, weights)[0]


def reference(x, dy, w_gate, w_up, w_down, m_w_gate, m_w_up, m_w_down, v_w_gate, v_w_up, v_w_down):
    weights = dict(zip(NAMES, (w_gate, w_up, w_down), strict=True))

    def take(so_far, sequence):
        h, by_y = sequence
        _, back = jax.vjp(lambda w: stack(w, h), weights)
        return jax.tree.map(lambda total, term: total + term.astype(jnp.float32), so_far, back(by_y)[0]), None

    none_yet = {name: jnp.zeros(w.shape, jnp.float32) for name, w in weights.items()}
    by_weights, _ = lax.scan(take, none_yet, (x, dy))
    gradients = [by_weights[name].astype(jnp.bfloat16).astype(jnp.float32) for name in NAMES]
    new = [
        adamw(w.astype(jnp.float32), m, v, g)
        for w, m, v, g in zip((w_gate, w_up, w_down), (m_w_gate, m_w_up, m_w_down), (v_w_gate, v_w_up, v_w_down), gradients, strict=True)
    ]
    return tuple(one[which] for which in range(3) for one in new)
```

```python
import functools

import jax
import jax.numpy as jnp
from jax import lax
from jax.experimental import pallas as pl
from jax.experimental.pallas import tpu as pltpu
from jax.sharding import PartitionSpec as P


BF, F32 = jnp.bfloat16, jnp.float32
AXES = ("rep", "dp")
MESH = pl.DeviceIdType.MESH
CHUNK = 512
ROWS = 512
ADAM_COLS = 256
VMEM = 60 << 20
NX = 5


def sigmoid(x):
    return pl.reciprocal(1.0 + jnp.exp(-x), approx=False)

def nn(a, b):
    return jnp.dot(a, b, preferred_element_type=F32)

def nt(a, b):
    return lax.dot_general(a, b, (((1,), (1,)), ((), ())), preferred_element_type=F32)

def tn(a, b):
    return lax.dot_general(a, b, (((0,), (0,)), ((), ())), preferred_element_type=F32)

def scale_of(wide):
    return lax.rsqrt(jnp.mean(wide * wide, -1, keepdims=True) + 1e-6)

def normed(h):
    wide = h.astype(F32)
    return (wide * scale_of(wide)).astype(BF)

def forward_kernel(rows_, h_ref, wg_ref, wu_ref, wd_ref, out_ref, a_ref, next_ref, gate_ref, up_ref, acc_ref):
    step = pl.program_id(0)

    @pl.when(step == 0)
    def _():
        a_ref[...] = normed(h_ref[...])
        acc_ref[...] = jnp.zeros_like(acc_ref)

    for r in range(h_ref.shape[0] // rows_):
        rows = pl.ds(r * rows_, rows_)
        a = a_ref[rows]
        gate = nn(a, wg_ref[...])
        up = nn(a, wu_ref[...])
        gate_ref[rows] = gate
        up_ref[rows] = up
        p = (gate * sigmoid(gate) * up).astype(BF)
        acc_ref[rows] += nn(p, wd_ref[...])

    @pl.when(step == pl.num_programs(0) - 1)
    def _():
        h = h_ref[...] + acc_ref[...].astype(BF)
        out_ref[...] = h
        next_ref[...] = normed(h)

def forward(h, wg, wu, wd, layer, chunk=512, rows=512):
    t, d = h.shape
    ff = wg.shape[2]
    full = pl.BlockSpec((t, d), lambda j: (0, 0))
    wide = pl.BlockSpec((None, d, chunk), lambda j: (layer, 0, j))
    cols = pl.BlockSpec((t, chunk), lambda j: (0, j))
    return pl.pallas_call(
        functools.partial(forward_kernel, rows),
        grid=(ff // chunk,),
        in_specs=[full, wide, wide, pl.BlockSpec((None, chunk, d), lambda j: (layer, j, 0))],
        out_specs=[full] * 3 + [cols] * 2,
        out_shape=[jax.ShapeDtypeStruct((t, d), BF)] * 3 + [jax.ShapeDtypeStruct((t, ff), F32)] * 2,
        scratch_shapes=[pltpu.VMEM((t, d), F32)],
        compiler_params=pltpu.CompilerParams(vmem_limit_bytes=VMEM),
        cost_estimate=pl.CostEstimate(flops=6 * t * d * ff, bytes_accessed=8 * t * ff, transcendentals=0),
        name="forward",
    )(h, wg, wu, wd)

def middle(gate, up, dp, rows, p_s, dg_s, du_s):
    dp = dp.astype(BF).astype(F32)
    s = sigmoid(gate)
    silu = gate * s
    p_s[rows] = (silu * up).astype(BF)
    du_s[rows] = (dp * silu).astype(BF)
    dg_s[rows] = (dp * up * (s + silu * (1.0 - s))).astype(BF)

def both_kernel(nx, a1, h1, dy, a0, wg, wu, wd, gate0, up0, *refs):
    n = 2 * (wd.shape[1] // 2 // CHUNK)
    refs = list(refs)
    take = lambda k: [refs.pop(0) for _ in range(k)]
    sums, came = take(n), take(nx)
    (landed,) = take(1)
    a_v, dy_v, b_v, da_v, p_s, dg_s, du_s, wg_v, wu_v, wd_v, gate_v, up_v, add_v, grad_v = take(14)
    in_sem, w_sem, g_sem, add_sem, out_sem, d_send, d_recv, x_send, x_recv = take(9)
    per = n // 2
    half_steps = 2 * per
    steps = 2 * half_steps
    j = pl.program_id(0)
    rep, dp = lax.axis_index("rep"), lax.axis_index("dp")
    core = lax.rem(dp, 2)
    beside = (rep, dp + 1 - 2 * core)
    across = (rep, lax.rem(dp + 2, 4))
    t = a_v.shape[0]

    def what(j):
        layer = j // half_steps
        k = lax.rem(j, half_steps)
        own = ((k >= 2) & (lax.rem(k, 2) == 0)) | (k == half_steps - 1)
        number = jnp.where(own, jnp.where(k == half_steps - 1, per - 1, k // 2 - 1), (k + 1) // 2)
        return layer, own, number, layer * per + number

    def columns(j):
        _, own, number, _ = what(j)
        side = jnp.where(own, core, 1 - core)
        return pl.ds(pl.multiple_of((side * per + number) * CHUNK, CHUNK), CHUNK)

    def loads(j, top):
        s = lax.rem(j, 2)
        cols = columns(j)
        if top:
            return [
                pltpu.make_async_copy(wg.at[1, :, cols], wg_v.at[s], w_sem.at[s, 0]),
                pltpu.make_async_copy(wu.at[1, :, cols], wu_v.at[s], w_sem.at[s, 1]),
                pltpu.make_async_copy(wd.at[1, cols], wd_v.at[s], w_sem.at[s, 2]),
            ]
        return [
            pltpu.make_async_copy(gate0.at[:, cols], gate_v.at[s], g_sem.at[s, 0]),
            pltpu.make_async_copy(up0.at[:, cols], up_v.at[s], g_sem.at[s, 1]),
            pltpu.make_async_copy(wd.at[0, cols], wd_v.at[s], w_sem.at[s, 2]),
        ]

    def load(j, do):
        @pl.when(j < half_steps)
        def _():
            for c in loads(j, True):
                do(c)

        @pl.when((j >= half_steps) & (j < steps))
        def _():
            for c in loads(j, False):
                do(c)

    start, wait = (lambda c: c.start()), (lambda c: c.wait())
    slot = lax.rem(j, 2)

    def d2d(q, s):
        return pltpu.make_async_remote_copy(
            src_ref=grad_v.at[s], dst_ref=landed.at[q], send_sem=d_send.at[q], recv_sem=d_recv.at[q], device_id=beside, device_id_type=MESH)

    def exchange(k):
        return pltpu.make_async_remote_copy(
            src_ref=sums[k], dst_ref=came[k], send_sem=x_send.at[k], recv_sem=x_recv.at[k], device_id=across, device_id_type=MESH)

    def add_copy(q, s):
        return pltpu.make_async_copy(landed.at[q], add_v.at[s], add_sem.at[s])

    def ship(j):
        _, own, _, q = what(j)
        s = lax.rem(j, 2)
        pl.when(jnp.logical_not(own))(lambda: d2d(q, s).start())
        for k in range(n):
            @pl.when(own & (q == k))
            def _():
                c = pltpu.make_async_copy(grad_v.at[s], sums[k], out_sem)
                c.start()
                c.wait()
                if k < nx:
                    exchange(k).start()

    first_loads = [(a1, a_v), (dy, dy_v), (h1, b_v)]

    @pl.when(j == 0)
    def _():
        load(j, start)
        for k, (src, dst) in enumerate(first_loads):
            pltpu.make_async_copy(src, dst, in_sem.at[k]).start()
        barrier = pltpu.get_barrier_semaphore()
        for device in (beside, across):
            pl.semaphore_signal(barrier, inc=1, device_id=device, device_id_type=MESH)
        pl.semaphore_wait(barrier, 2)
        add_v[...] = jnp.zeros_like(add_v)
        for k, (src, dst) in enumerate(first_loads):
            pltpu.make_async_copy(src, dst, in_sem.at[k]).wait()

    @pl.when(j >= 2)
    def _():
        _, own, _, q = what(j - 2)
        pl.when(jnp.logical_not(own))(lambda: d2d(q, slot).wait_send())

    pl.when(j >= 1)(lambda: ship(j - 1))
    load(j, wait)
    load(j + 1, start)

    def own_at(j):
        return (j < steps) & what(j)[1]

    @pl.when(own_at(j))
    def _():
        add_copy(what(j)[3], slot).wait()

    @pl.when(jnp.logical_not(own_at(j)))
    def _():
        add_v[slot] = jnp.zeros(add_v.shape[1:], BF)

    @pl.when(own_at(j + 1))
    def _():
        q = what(j + 1)[3]
        d2d(q, slot).wait_recv()
        add_copy(q, 1 - slot).start()

    def gradients(left_a):
        for k, (left, right) in enumerate(((left_a, dg_s), (left_a, du_s), (dy_v, p_s))):
            grad_v[slot, k] = (tn(left[...], right[...]) + add_v[slot, k].astype(F32)).astype(BF)

    @pl.when(j < half_steps)
    def _():
        wgj, wuj, wdj = wg_v.at[slot], wu_v.at[slot], wd_v.at[slot]
        for r in range(t // ROWS):
            rows = pl.ds(r * ROWS, ROWS)
            a = a_v[rows]
            middle(nn(a, wgj[...]), nn(a, wuj[...]), nt(dy_v[rows], wdj[...]), rows, p_s, dg_s, du_s)
        gradients(a_v)
        for r in range(t // ROWS):
            rows = pl.ds(r * ROWS, ROWS)
            da_v[rows] = jnp.where(j == 0, 0.0, da_v[rows]) + (nt(dg_s[rows], wgj[...]) + nt(du_s[rows], wuj[...]))

    @pl.when(j == half_steps - 1)
    def _():
        def turn(r, _):
            rows = pl.ds(pl.multiple_of(r * 256, 256), 256)
            wide = b_v[rows].astype(F32)
            da = da_v[rows].astype(BF).astype(F32)
            scale = scale_of(wide)
            dot = jnp.sum(da * wide, -1, keepdims=True)
            dwide = da * scale - wide * (scale * scale * scale * dot * (1.0 / wide.shape[-1]))
            dy_v[rows] = dy_v[rows] + dwide.astype(BF)
            return 0

        lax.fori_loop(0, t // 256, turn, 0)
        c = pltpu.make_async_copy(a0, a_v, in_sem.at[0])
        c.start()
        c.wait()

    @pl.when(j >= half_steps)
    def _():
        gj, uj, wdj = gate_v.at[slot], up_v.at[slot], wd_v.at[slot]
        for r in range(t // ROWS):
            rows = pl.ds(r * ROWS, ROWS)
            middle(gj[rows], uj[rows], nt(dy_v[rows], wdj[...]), rows, p_s, dg_s, du_s)
        gradients(a_v)

    @pl.when(j == steps - 1)
    def _():
        ship(j)
        for k in range(nx):
            exchange(k).wait()

def both(a1, h1, dy, a0, weights, saved, nx):
    t, d = a1.shape
    ff = weights[2].shape[1]
    n = 2 * (ff // 2 // CHUNK)
    anywhere = pl.BlockSpec(memory_space=pl.ANY)
    chunk = jax.ShapeDtypeStruct((3, d, CHUNK), BF)
    outs = [chunk] * (n + nx) + [jax.ShapeDtypeStruct((n, 3, d, CHUNK), BF)]
    out = pl.pallas_call(
        functools.partial(both_kernel, nx),
        grid=(2 * n,),
        in_specs=[anywhere] * 9,
        out_specs=[anywhere] * len(outs),
        out_shape=outs,
        scratch_shapes=[pltpu.VMEM((t, d), BF)] * 3 + [pltpu.VMEM((t, d), F32)] + [pltpu.VMEM((t, CHUNK), BF)] * 3
        + [pltpu.VMEM((2, d, CHUNK), BF)] * 2 + [pltpu.VMEM((2, CHUNK, d), BF)] + [pltpu.VMEM((2, t, CHUNK), F32)] * 2
        + [pltpu.VMEM((2, 3, d, CHUNK), BF)] * 2
        + [pltpu.SemaphoreType.DMA((3,)), pltpu.SemaphoreType.DMA((2, 3)), pltpu.SemaphoreType.DMA((2, 2)), pltpu.SemaphoreType.DMA((2,)), pltpu.SemaphoreType.DMA]
        + [pltpu.SemaphoreType.DMA((n,))] * 2 + [pltpu.SemaphoreType.DMA((max(nx, 1),))] * 2,
        compiler_params=pltpu.CompilerParams(vmem_limit_bytes=67_000_000, collective_id=1, has_side_effects=True),
        cost_estimate=pl.CostEstimate(flops=24 * t * d * ff, bytes_accessed=8 * t * ff, transcendentals=0),
        name="backward",
    )(a1, h1, dy, a0, *weights, *saved)
    return out[:n], out[n : n + nx]


def adamw_kernel(own, aliased, chunks, off_ref, *refs):
    gs, refs = refs[: (1 + own) * chunks], refs[(1 + own) * chunks :]
    w, m, v = refs[0:3], refs[3:6], refs[6:9]
    refs = refs[9 + 9 * aliased :]
    new_w, new_m, new_v = refs[0:3], refs[3:6], refs[6:9]

    def work(g_refs):
        for i in range(3):
            g = g_refs[0][i].astype(F32)
            if own:
                total = (g + g_refs[1][i].astype(F32)).astype(BF)
                refs[9][i] = total
                g = total.astype(F32)
            if i == 2:
                g = g.T
            mi = 0.9 * m[i][...] + 0.1 * g
            vi = 0.95 * v[i][...] + 0.05 * g * g
            wi = w[i][...].astype(F32)
            step = mi * lax.rsqrt(vi + 1e-8) + 0.1 * wi
            new_w[i][...] = (wi - 0.02 * step).astype(BF)
            new_m[i][...] = mi
            new_v[i][...] = vi

    per = CHUNK // ADAM_COLS
    for k in range(chunks if own else 1):
        g_refs = gs[k * (1 + own) : (k + 1) * (1 + own)]
        if own and chunks > 1:
            pl.when(pl.program_id(0) // per == k)(functools.partial(work, g_refs))
        else:
            work(g_refs)


def adamw(off, gs, weights, m, v, new, layer, own):
    d, unit = gs[0].shape[1:]
    chunks = len(gs) // 2 if own else 1
    unit *= chunks
    per = CHUNK // ADAM_COLS
    wide = pl.BlockSpec((None, d, ADAM_COLS), lambda j, o: (layer, 0, o[0] + j))
    tall = pl.BlockSpec((None, ADAM_COLS, d), lambda j, o: (layer, o[0] + j, 0))
    grad = pl.BlockSpec((3, d, ADAM_COLS), lambda j, o: (0, 0, j))

    def part(k):
        return pl.BlockSpec((3, d, ADAM_COLS), lambda j, o: (0, 0, jnp.clip(j - k * per, 0, per - 1)))

    kinds = [wide, wide, tall] * 3
    shapes = [jax.ShapeDtypeStruct(x.shape, x.dtype) for x in (*weights, *m, *v)]
    out = pl.pallas_call(
        functools.partial(adamw_kernel, own, new is not None, chunks),
        grid_spec=pltpu.PrefetchScalarGridSpec(
            num_scalar_prefetch=1,
            grid=(unit // ADAM_COLS,),
            in_specs=([part(k // 2) for k in range(2 * chunks)] if own else [grad])
            + kinds
            + ([pl.BlockSpec(memory_space=pl.ANY)] * 9 if new is not None else []),
            out_specs=kinds + [grad] * own,
        ),
        out_shape=shapes + [jax.ShapeDtypeStruct((3, d, unit), BF)] * own,
        input_output_aliases={10 + len(gs) + i: i for i in range(9)} if new is not None else {},
        compiler_params=pltpu.CompilerParams(vmem_limit_bytes=VMEM),
        cost_estimate=pl.CostEstimate(flops=int(8 * 3 * d * unit * 30), bytes_accessed=22 * 3 * d * unit, transcendentals=0),
        name="adamw_own" if own else "adamw_other",
    )(off, *gs, *weights, *m, *v, *(new or ()))
    return out[:9], out[9:]


ORDER = (
    "F", "G", "x5", "x6", "A0+1", "h0", "A2+3", "h2", "B0+1", "x7", "B2+3", "x8",
    "A4", "h4", "A5", "h5", "B4", "x9", "B5", "x10", "A6+7", "h6", "x11", "B6+7",
    "A8", "h8", "A9", "h9", "B8", "B9", "A10", "h10", "A11", "h11", "B10", "B11",
)


def chunks_of(name):
    first, *more = name[1:].split("+")
    return range(int(first), 1 + int(more[0] if more else first))


def solution(mesh):
    reps, dps = mesh.shape["rep"], mesh.shape["dp"]

    def pairs(to):
        return [(r * dps + i, r * dps + to(i)) for r in range(reps) for i in range(dps)]

    across = pairs(lambda i: (i + 2) % dps)
    beside = pairs(lambda i: i ^ 1)

    def step(x, dy, *arrays):
        weights, m, v = (arrays[i : i + 3] for i in (0, 3, 6))
        core = lax.axis_index("dp") % 2
        half = weights[0].shape[2] // 2
        per = half // CHUNK
        have = {}
        new = None

        def offset(side, number):
            return ((side * half + number * CHUNK) // ADAM_COLS).astype(jnp.int32).reshape(1)

        def send(z, to):
            return lax.ppermute(z, AXES, to)

        for name in ORDER:
            kind = name[0]
            if kind == "F":
                h1, a0, a1, gate0, up0 = forward(x[0], *weights, 0)
            elif kind == "G":
                sums, came = both(a1, h1, dy[0], a0, weights, (gate0, up0), NX)
                came = list(came) + [None] * (2 * per - NX)
            elif kind == "x":
                k = int(name[1:])
                came[k] = send(sums[k], across)
            elif kind == "h":
                have[name[1:]] = send(have["A" + name[1:]], beside)
            else:
                ks = chunks_of(name)
                layer, number, first = 1 - ks[0] // per, ks[0] % per, str(ks[0])
                if kind == "A":
                    gs = [z for k in ks for z in (sums[k], came[k])]
                    new, (have["A" + first],) = adamw(offset(core, number), gs, weights, m, v, new, layer, 1)
                else:
                    new, _ = adamw(offset(1 - core, number), [have[first]], weights, m, v, new, layer, 0)
        return tuple(new)

    return jax.shard_map(
        step,
        mesh=mesh,
        in_specs=(P(("rep", "dp"), None, None),) * 2 + (P(None, None, None),) * 9,
        out_specs=(P("rep", None, None),) * 9,
        check_vma=False,
    )
```

```python
import functools

import jax
import jax.numpy as jnp
from jax import lax
from jax.experimental import pallas as pl
from jax.experimental.pallas import tpu as pltpu
from jax.sharding import PartitionSpec as P


BF, F32 = jnp.bfloat16, jnp.float32
AXES = ("rep", "dp")
MESH = pl.DeviceIdType.MESH
CHUNK = 512
ROWS = 512
ADAM_COLS = 256
VMEM = 60 << 20
NEAR = 4
NX = 4


def sigmoid(x):
    return pl.reciprocal(1.0 + jnp.exp(-x), approx=False)


def nn(a, b):
    return jnp.dot(a, b, preferred_element_type=F32)


def nt(a, b):
    return lax.dot_general(a, b, (((1,), (1,)), ((), ())), preferred_element_type=F32)


def tn(a, b):
    return lax.dot_general(a, b, (((0,), (0,)), ((), ())), preferred_element_type=F32)


def scale_of(wide):
    return lax.rsqrt(jnp.mean(wide * wide, -1, keepdims=True) + 1e-6)


def normed(h):
    wide = h.astype(F32)
    return (wide * scale_of(wide)).astype(BF)


def forward_kernel(rows_, h_ref, wg_ref, wu_ref, wd_ref, out_ref, a_ref, next_ref, gate_ref, up_ref, acc_ref):
    step = pl.program_id(0)

    @pl.when(step == 0)
    def _():
        a_ref[...] = normed(h_ref[...])
        acc_ref[...] = jnp.zeros_like(acc_ref)

    for r in range(h_ref.shape[0] // rows_):
        rows = pl.ds(r * rows_, rows_)
        a = a_ref[rows]
        gate = nn(a, wg_ref[...])
        up = nn(a, wu_ref[...])
        gate_ref[rows] = gate
        up_ref[rows] = up
        p = (gate * sigmoid(gate) * up).astype(BF)
        acc_ref[rows] += nn(p, wd_ref[...])

    @pl.when(step == pl.num_programs(0) - 1)
    def _():
        h = h_ref[...] + acc_ref[...].astype(BF)
        out_ref[...] = h
        next_ref[...] = normed(h)


def forward(h, wg, wu, wd, layer, chunk=512, rows=512):
    t, d = h.shape
    ff = wg.shape[2]
    full = pl.BlockSpec((t, d), lambda j: (0, 0))
    wide = pl.BlockSpec((None, d, chunk), lambda j: (layer, 0, j))
    cols = pl.BlockSpec((None, t, chunk), lambda j: (j, 0, 0))
    return pl.pallas_call(
        functools.partial(forward_kernel, rows),
        grid=(ff // chunk,),
        in_specs=[full, wide, wide, pl.BlockSpec((None, chunk, d), lambda j: (layer, j, 0))],
        out_specs=[full] * 3 + [cols] * 2,
        out_shape=[jax.ShapeDtypeStruct((t, d), BF)] * 3 + [jax.ShapeDtypeStruct((ff // chunk, t, chunk), F32)] * 2,
        scratch_shapes=[pltpu.VMEM((t, d), F32)],
        compiler_params=pltpu.CompilerParams(vmem_limit_bytes=VMEM),
        cost_estimate=pl.CostEstimate(flops=6 * t * d * ff, bytes_accessed=8 * t * ff, transcendentals=0),
        name="forward",
    )(h, wg, wu, wd)


def middle(gate, up, dp, rows, p_s, dg_s, du_s):
    dp = dp.astype(BF).astype(F32)
    s = sigmoid(gate)
    silu = gate * s
    p_s[rows] = (silu * up).astype(BF)
    du_s[rows] = (dp * silu).astype(BF)
    dg_s[rows] = (dp * up * (s + silu * (1.0 - s))).astype(BF)


def both_kernel(near, nx, a1, h1, dy, a0, wg, wu, wd, gate0, up0, *refs):
    per = wd.shape[1] // 2 // CHUNK
    far = per - near
    n = near + per
    refs = list(refs)
    take = lambda k: [refs.pop(0) for _ in range(k)]
    stacked, came, *sums = take(2 + n - nx)
    sums = [stacked.at[k] for k in range(nx)] + sums
    (landed,) = take(1)
    saved = take(3)
    (peer_a,) = take(1)
    a_v, dy_v, b_v, da_v, p_s, dg_s, du_s, wg_v, wu_v, wd_v, gate_v, up_v, add_v, grad_v = take(14)
    in_sem, w_sem, g_sem, add_sem, out_sem, save_sem, d_send, d_recv, x_send, x_recv, a_send, a_recv = take(12)
    t_save, t_low, steps = 2 * near, 2 * per, 4 * per
    j = pl.program_id(0)
    rep, dp = lax.axis_index("rep"), lax.axis_index("dp")
    core = lax.rem(dp, 2)
    beside = (rep, dp + 1 - 2 * core)
    across = (rep, lax.rem(dp + 2, 4))
    t = a_v.shape[0]

    def saving(j):
        return (j >= t_save) & (j < t_low)

    def what(j):
        low = j >= t_low
        m = jnp.where(low, per, near)
        k = jnp.where(low, j - t_low, j)
        own = ((k >= 2) & (lax.rem(k, 2) == 0)) | (k == 2 * m - 1)
        number = jnp.where(own, jnp.where(k == 2 * m - 1, m - 1, k // 2 - 1), (k + 1) // 2)
        return own & jnp.logical_not(saving(j)), number, jnp.where(low, near, 0) + number

    def gives(j, own):
        mine = what(j)[0]
        return (j < steps) & jnp.logical_not(saving(j)) & (mine if own else jnp.logical_not(mine))

    def block_of(j):
        own, number, _ = what(j)
        side = jnp.where(own, core, 1 - core)
        k = j - t_save
        near_block = side * per + number
        return jnp.where(saving(j), (k // far) * per + near + lax.rem(k, far), near_block) if far else near_block

    def loads(j, top):
        s = lax.rem(j, 2)
        block = block_of(j)
        cols = pl.ds(pl.multiple_of(block * CHUNK, CHUNK), CHUNK)
        if top:
            return [
                pltpu.make_async_copy(wg.at[1, :, cols], wg_v.at[s], w_sem.at[s, 0]),
                pltpu.make_async_copy(wu.at[1, :, cols], wu_v.at[s], w_sem.at[s, 1]),
                pltpu.make_async_copy(wd.at[1, cols], wd_v.at[s], w_sem.at[s, 2]),
            ]
        return [
            pltpu.make_async_copy(gate0.at[block], gate_v.at[s], g_sem.at[s, 0]),
            pltpu.make_async_copy(up0.at[block], up_v.at[s], g_sem.at[s, 1]),
            pltpu.make_async_copy(wd.at[0, cols], wd_v.at[s], w_sem.at[s, 2]),
        ]

    def load(j, do):
        @pl.when(j < t_low)
        def _():
            for c in loads(j, True):
                do(c)

        @pl.when((j >= t_low) & (j < steps))
        def _():
            for c in loads(j, False):
                do(c)

    start, wait = (lambda c: c.start()), (lambda c: c.wait())
    slot = lax.rem(j, 2)

    def d2d(q, s):
        return pltpu.make_async_remote_copy(
            src_ref=grad_v.at[s], dst_ref=landed.at[q], send_sem=d_send.at[q], recv_sem=d_recv.at[q], device_id=beside, device_id_type=MESH
        )

    def exchange(k):
        return pltpu.make_async_remote_copy(
            src_ref=sums[k], dst_ref=came.at[k], send_sem=x_send.at[k], recv_sem=x_recv.at[k], device_id=across, device_id_type=MESH
        )

    states = pltpu.make_async_remote_copy(
        src_ref=a1, dst_ref=peer_a, send_sem=a_send, recv_sem=a_recv, device_id=across, device_id_type=MESH
    )

    def add_copy(q, s):
        return pltpu.make_async_copy(landed.at[q], add_v.at[s], add_sem.at[s])

    def saves(j, s):
        return [pltpu.make_async_copy(z.at[s], out.at[j - t_save], save_sem.at[s, i]) for i, (z, out) in enumerate(zip((dg_s, du_s, p_s), saved))]

    def late(j):
        low = j >= t_low
        k = jnp.where(low, j - t_low, j)
        return (k == 2) | (k == jnp.where(low, t_low, t_save) - 1)

    def keep(j, do, k_max):
        q = what(j)[2]
        s = lax.rem(j, 2)
        for k in range(k_max):
            pl.when(gives(j, True) & (q == k))(lambda k=k: do(k, s))

    def kept(k, s):
        return pltpu.make_async_copy(grad_v.at[s], sums[k], out_sem.at[s])

    def ship(j):
        pl.when(gives(j, False))(lambda: d2d(what(j)[2], lax.rem(j, 2)).start())
        keep(j, lambda k, s: kept(k, s).start(), n)
        if far:

            @pl.when(saving(j))
            def _():
                for c in saves(j, lax.rem(j, 2)):
                    c.start()

    def settle(j):
        pl.when(gives(j, False))(lambda: d2d(what(j)[2], lax.rem(j, 2)).wait_send())

        def done(k, s):
            kept(k, s).wait()
            if k < nx:
                exchange(k).start()

        keep(j, done, n)
        if far:

            @pl.when(saving(j))
            def _():
                for c in saves(j, lax.rem(j, 2)):
                    c.wait()

    first_loads = [(a1, a_v), (dy, dy_v), (h1, b_v)]

    @pl.when(j == 0)
    def _():
        load(j, start)
        for k, (src, dst) in enumerate(first_loads):
            pltpu.make_async_copy(src, dst, in_sem.at[k]).start()
        barrier = pltpu.get_barrier_semaphore()
        for device in (beside, across):
            pl.semaphore_signal(barrier, inc=1, device_id=device, device_id_type=MESH)
        pl.semaphore_wait(barrier, 2)
        states.start()
        for k, (src, dst) in enumerate(first_loads):
            pltpu.make_async_copy(src, dst, in_sem.at[k]).wait()

    pl.when(j >= 2)(lambda: settle(j - 2))
    pl.when(j >= 1)(lambda: ship(j - 1))
    load(j, wait)
    load(j + 1, start)

    def fetch(j):
        q = what(j)[2]
        d2d(q, lax.rem(j, 2)).wait_recv()
        add_copy(q, lax.rem(j, 2)).start()

    pl.when(gives(j, True) & late(j))(lambda: fetch(j))
    pl.when(gives(j, True))(lambda: add_copy(what(j)[2], slot).wait())
    pl.when(gives(j + 1, True) & jnp.logical_not(late(j + 1)))(lambda: fetch(j + 1))

    @pl.when(gives(j, False))
    def _():
        add_v[slot] = jnp.zeros(add_v.shape[1:], BF)

    p_j, dg_j, du_j = p_s.at[slot], dg_s.at[slot], du_s.at[slot]

    def gradients():
        for k, (left, right) in enumerate(((a_v, dg_j), (a_v, du_j), (dy_v, p_j))):
            grad_v[slot, k] = (tn(left[...], right[...]) + add_v[slot, k].astype(F32)).astype(BF)

    def upper(grads):
        wgj, wuj, wdj = wg_v.at[slot], wu_v.at[slot], wd_v.at[slot]
        for r in range(t // ROWS):
            rows = pl.ds(r * ROWS, ROWS)
            a = a_v[rows]
            middle(nn(a, wgj[...]), nn(a, wuj[...]), nt(dy_v[rows], wdj[...]), rows, p_j, dg_j, du_j)
        if grads:
            gradients()
        for r in range(t // ROWS):
            rows = pl.ds(r * ROWS, ROWS)
            da_v[rows] = jnp.where(j == 0, 0.0, da_v[rows]) + (nt(dg_j[rows], wgj[...]) + nt(du_j[rows], wuj[...]))

    pl.when(j < t_save)(lambda: upper(True))
    if far:
        pl.when(saving(j))(lambda: upper(False))

    @pl.when(j == t_low - 1)
    def _():
        def turn(r, _):
            rows = pl.ds(pl.multiple_of(r * 256, 256), 256)
            wide = b_v[rows].astype(F32)
            da = da_v[rows].astype(BF).astype(F32)
            scale = scale_of(wide)
            dot = jnp.sum(da * wide, -1, keepdims=True)
            dwide = da * scale - wide * (scale * scale * scale * dot * (1.0 / wide.shape[-1]))
            dy_v[rows] = dy_v[rows] + dwide.astype(BF)
            return 0

        lax.fori_loop(0, t // 256, turn, 0)
        c = pltpu.make_async_copy(a0, a_v, in_sem.at[0])
        c.start()
        c.wait()

    @pl.when(j >= t_low)
    def _():
        gj, uj, wdj = gate_v.at[slot], up_v.at[slot], wd_v.at[slot]
        for r in range(t // ROWS):
            rows = pl.ds(r * ROWS, ROWS)
            middle(gj[rows], uj[rows], nt(dy_v[rows], wdj[...]), rows, p_j, dg_j, du_j)
        gradients()

    @pl.when(j == steps - 1)
    def _():
        ship(j)
        settle(j - 1)
        settle(j)
        for k in range(nx):
            exchange(k).wait()
        states.wait()


def both(a1, h1, dy, a0, weights, saved, near, nx):
    t, d = a1.shape
    ff = weights[2].shape[1]
    per = ff // 2 // CHUNK
    n = near + per
    anywhere = pl.BlockSpec(memory_space=pl.ANY)
    chunk = jax.ShapeDtypeStruct((3, d, CHUNK), BF)
    kept = jax.ShapeDtypeStruct((2 * (per - near), t, CHUNK), BF)
    stack = jax.ShapeDtypeStruct((nx, 3, d, CHUNK), BF)
    outs = [stack] * 2 + [chunk] * (n - nx) + [jax.ShapeDtypeStruct((n, 3, d, CHUNK), BF)] + [kept] * 3 + [jax.ShapeDtypeStruct((t, d), BF)]
    dma = pltpu.SemaphoreType.DMA
    out = pl.pallas_call(
        functools.partial(both_kernel, near, nx),
        grid=(4 * per,),
        in_specs=[anywhere] * 9,
        out_specs=[anywhere] * len(outs),
        out_shape=outs,
        scratch_shapes=[pltpu.VMEM((t, d), BF)] * 3
        + [pltpu.VMEM((t, d), F32)]
        + [pltpu.VMEM((2, t, CHUNK), BF)] * 3
        + [pltpu.VMEM((2, d, CHUNK), BF)] * 2
        + [pltpu.VMEM((2, CHUNK, d), BF)]
        + [pltpu.VMEM((2, t, CHUNK), F32)] * 2
        + [pltpu.VMEM((2, 3, d, CHUNK), BF)] * 2
        + [dma((3,)), dma((2, 3)), dma((2, 2)), dma((2,)), dma((2,)), dma((2, 3))]
        + [dma((n,))] * 2
        + [dma((nx,))] * 2
        + [dma, dma],
        compiler_params=pltpu.CompilerParams(vmem_limit_bytes=67_000_000, collective_id=1, has_side_effects=True),
        cost_estimate=pl.CostEstimate(flops=24 * t * d * ff, bytes_accessed=8 * t * ff, transcendentals=0),
        name="backward",
    )(a1, h1, dy, a0, *weights, *saved)
    return out[:2], [[z, None] for z in out[2 : 2 + n - nx]], out[3 + n - nx : 6 + n - nx], out[6 + n - nx]


def adamw_block(gs, w, m, v, new_w, new_m, new_v, sum_ref):
    for i in range(3):
        g = gs[0][i].astype(F32)
        if sum_ref is not None:
            total = (g + gs[1][i].astype(F32)).astype(BF)
            sum_ref[i] = total
            g = total.astype(F32)
        if i == 2:
            g = g.T
        mi = 0.9 * m[i][...] + 0.1 * g
        vi = 0.95 * v[i][...] + 0.05 * g * g
        wi = w[i][...].astype(F32)
        step = mi * lax.rsqrt(vi + 1e-8) + 0.1 * wi
        new_w[i][...] = (wi - 0.02 * step).astype(BF)
        new_m[i][...] = mi
        new_v[i][...] = vi


def shared_kernel(own, aliased, table_ref, a_own, a_peer, dy_own, dy_peer, dg, du, p, wg_ref, wu_ref, wd_ref, *refs):
    refs = list(refs)
    take = lambda k: [refs.pop(0) for _ in range(k)]
    add_ref = take(1)[0] if own else None
    gs = take(1 if own else 2)
    w, m, v = take(3), take(3), take(3)
    take(9 * aliased)
    (out_ref,) = take(1)
    new = take(3), take(3), take(3)
    sum_ref = None if own else take(1)[0]
    a_st, dy_st, dg_s, du_s, p_s, in_sem, save_sem = take(7)
    j, part = pl.program_id(0), pl.program_id(1)
    t = a_own.shape[0]
    width = wd_ref.shape[0]
    per = CHUNK // width
    here = table_ref[0, 0]
    mine = pl.multiple_of(here * t, t)
    theirs = pl.multiple_of((1 - here) * t, t)

    def saves():
        block = table_ref[2, j]
        cols = pl.ds(pl.multiple_of(lax.rem(block, per) * width, width), width)
        return [
            pltpu.make_async_copy(src.at[block // per, :, cols], dst.at[pl.ds(mine, t)], save_sem.at[i])
            for i, (src, dst) in enumerate(((dg, dg_s), (du, du_s), (p, p_s)))
        ]

    @pl.when((j == 0) & (part == 0))
    def _():
        copies = [
            pltpu.make_async_copy(src, dst.at[pl.ds(at, t)], in_sem.at[i])
            for i, (src, dst, at) in enumerate(((a_peer, a_st, theirs), (dy_peer, dy_st, theirs), (a_own, a_st, mine), (dy_own, dy_st, mine)))
        ]
        for c in copies:
            c.start()
        for c in copies:
            c.wait()

    @pl.when(part == 0)
    def _():
        for c in saves():
            c.start()
        for r in range(t // ROWS):
            rows = pl.ds(pl.multiple_of(theirs + r * ROWS, ROWS), ROWS)
            a = a_st[rows]
            middle(nn(a, wg_ref[...]), nn(a, wu_ref[...]), nt(dy_st[rows], wd_ref[...]), rows, p_s, dg_s, du_s)
        adamw_block(gs, w, m, v, *new, sum_ref)

    @pl.when(part == 1)
    def _():
        for c in saves():
            c.wait()
        for k, (left, right) in enumerate(((a_st, dg_s), (a_st, du_s), (dy_st, p_s))):
            g = tn(left[...], right[...])
            if own:
                g += add_ref[k].astype(F32)
            out_ref[k] = g.astype(BF)
        adamw_block(gs, w, m, v, *new, sum_ref)


def shared(table, a_own, a_peer, dy_own, dy_peer, saved, weights, add, gs, moments, new, steps, jobs):
    t, d = a_own.shape
    own = add is not None
    width = ADAM_COLS
    anywhere = pl.BlockSpec(memory_space=pl.ANY)
    wide = pl.BlockSpec((None, d, width), lambda j, p, c: (1, 0, c[1, j]))
    part = pl.BlockSpec((3, d, width), lambda j, p, c: (0, 0, j))

    def job(j, p):
        return jnp.minimum(2 * j + p, jobs - 1)

    stack = pl.BlockSpec((None, 3, d, width), lambda j, p, c: (c[5, job(j, p)], 0, 0, c[6, job(j, p)]))
    across = pl.BlockSpec((None, d, width), lambda j, p, c: (c[3, job(j, p)], 0, c[4, job(j, p)]))
    down = pl.BlockSpec((None, width, d), lambda j, p, c: (c[3, job(j, p)], c[4, job(j, p)], 0))
    kinds = [across, across, down] * 3
    arrays = (*weights, *moments)
    out = [jax.ShapeDtypeStruct((3, d, steps * width), BF)] + [jax.ShapeDtypeStruct(x.shape, x.dtype) for x in arrays]
    dma = pltpu.SemaphoreType.DMA
    before = 11 + own + len(gs) + 9
    out = pl.pallas_call(
        functools.partial(shared_kernel, own, new is not None),
        grid_spec=pltpu.PrefetchScalarGridSpec(
            num_scalar_prefetch=1,
            grid=(steps, 2),
            in_specs=[anywhere] * 7
            + [wide, wide, pl.BlockSpec((None, width, d), lambda j, p, c: (1, c[1, j], 0))]
            + [part] * own
            + [stack] * len(gs)
            + kinds
            + [anywhere] * (9 if new is not None else 0),
            out_specs=[part] + kinds + [stack] * (not own),
            scratch_shapes=[pltpu.VMEM((2 * t, d), BF)] * 2 + [pltpu.VMEM((2 * t, width), BF)] * 3 + [dma((4,)), dma((3,))],
        ),
        out_shape=out + [jax.ShapeDtypeStruct(gs[0].shape, BF)] * (not own),
        input_output_aliases={before + i: 1 + i for i in range(9)} if new is not None else {},
        compiler_params=pltpu.CompilerParams(vmem_limit_bytes=67_000_000),
        cost_estimate=pl.CostEstimate(flops=18 * t * d * width * steps, bytes_accessed=22 * 3 * d * width * jobs, transcendentals=0),
        name="shared_own" if own else "shared_other",
    )(table, a_own, a_peer, dy_own, dy_peer, *saved, *weights, *([add] if own else []), *gs, *arrays, *(new or ()))
    return out[0], out[1:10], out[10:]


def adamw_kernel(own, aliased, chunks, off_ref, *refs):
    gs, refs = refs[: (1 + own) * chunks], refs[(1 + own) * chunks :]
    w, m, v = refs[0:3], refs[3:6], refs[6:9]
    refs = refs[9 + 9 * aliased :]
    new_w, new_m, new_v = refs[0:3], refs[3:6], refs[6:9]

    def work(g_refs):
        adamw_block(g_refs, w, m, v, new_w, new_m, new_v, refs[9] if own else None)

    per = CHUNK // ADAM_COLS
    for k in range(chunks if own else 1):
        g_refs = gs[k * (1 + own) : (k + 1) * (1 + own)]
        if own and chunks > 1:
            pl.when(pl.program_id(0) // per == k)(functools.partial(work, g_refs))
        else:
            work(g_refs)


def adamw(off, gs, weights, m, v, new, layer, own):
    d = weights[0].shape[1]
    chunks = len(gs) // 2 if own else 1
    unit = chunks * gs[0].shape[2]
    per = CHUNK // ADAM_COLS
    wide = pl.BlockSpec((None, d, ADAM_COLS), lambda j, o: (layer, 0, o[0] + j))
    tall = pl.BlockSpec((None, ADAM_COLS, d), lambda j, o: (layer, o[0] + j, 0))
    grad = pl.BlockSpec((3, d, ADAM_COLS), lambda j, o: (0, 0, j))

    def part(k):
        return pl.BlockSpec((3, d, ADAM_COLS), lambda j, o: (0, 0, jnp.clip(j - k * per, 0, per - 1)))

    kinds = [wide, wide, tall] * 3
    shapes = [jax.ShapeDtypeStruct(x.shape, x.dtype) for x in (*weights, *m, *v)]
    out = pl.pallas_call(
        functools.partial(adamw_kernel, own, new is not None, chunks),
        grid_spec=pltpu.PrefetchScalarGridSpec(
            num_scalar_prefetch=1,
            grid=(unit // ADAM_COLS,),
            in_specs=([part(k // 2) for k in range(2 * chunks)] if own else [grad])
            + kinds
            + ([pl.BlockSpec(memory_space=pl.ANY)] * 9 if new is not None else []),
            out_specs=kinds + [grad] * own,
        ),
        out_shape=shapes + [jax.ShapeDtypeStruct((3, d, unit), BF)] * own,
        input_output_aliases={10 + len(gs) + i: i for i in range(9)} if new is not None else {},
        compiler_params=pltpu.CompilerParams(vmem_limit_bytes=VMEM),
        cost_estimate=pl.CostEstimate(flops=int(8 * 3 * d * unit * 30), bytes_accessed=22 * 3 * d * unit, transcendentals=0),
        name="adamw_own" if own else "adamw_other",
    )(off, *gs, *weights, *m, *v, *(new or ()))
    return out[:9], out[9:]


ORDER = (
    "p0", "F", "G", "x4", "x5", "Y0", "s0", "t0", "x6", "x7", "Z0", "k0",
    "x8", "A4+5", "h4", "x9", "C0", "B4+5", "D0", "A6", "h6", "A7", "h7", "B6",
    "B7", "A8", "h8", "A9", "h9", "B8", "B9",
)


def chunks_of(name):
    first, *more = name[1:].split("+")
    return range(int(first), 1 + int(more[0] if more else first))


def solution(mesh):
    reps, dps = mesh.shape["rep"], mesh.shape["dp"]

    def pairs(to):
        return [(r * dps + i, r * dps + to(i)) for r in range(reps) for i in range(dps)]

    across = pairs(lambda i: (i + 2) % dps)
    beside = pairs(lambda i: i ^ 1)

    def step(x, dy, *arrays):
        weights, m, v = (arrays[i : i + 3] for i in (0, 3, 6))
        core = lax.axis_index("dp") % 2
        half = weights[0].shape[2] // 2
        per = half // CHUNK
        have = {}
        new = None

        def offset(side, number):
            return ((side * half + number * CHUNK) // ADAM_COLS).astype(jnp.int32).reshape(1)

        def send(z, to):
            return lax.ppermute(z, AXES, to)

        def table(side):
            far, parts = per - NEAR, CHUNK // ADAM_COLS
            k = jnp.arange(far * parts, dtype=jnp.int32)
            i = jnp.arange(NX * parts, dtype=jnp.int32)
            chunk, layer = i // parts, (i // parts < NEAR).astype(jnp.int32)
            number = chunk - (1 - layer) * NEAR
            rows = [where, (side * per + NEAR) * parts + k, side * far * parts + k, layer, (side * per + number) * parts + i % parts, chunk, i % parts]
            width = max(far, NX) * parts
            return jnp.stack([jnp.pad(r.astype(jnp.int32), (0, width - r.shape[0])) for r in rows])

        where = (lax.axis_index("dp") // 2).astype(jnp.int32).reshape(1)
        moments = (*m, *v)
        steps, jobs = (per - NEAR) * (CHUNK // ADAM_COLS), NX * (CHUNK // ADAM_COLS)
        for name in ORDER:
            kind = name[0]
            if kind == "p":
                peer_dy = send(dy[0], across)
            elif kind == "F":
                h1, a0, a1, gate0, up0 = forward(x[0], *weights, 0)
            elif kind == "G":
                stacks, pair, saved, peer_a = both(a1, h1, dy[0], a0, weights, (gate0, up0), NEAR, NX)
            elif kind == "Y":
                sides = jnp.concatenate([table(1 - core)[:3], table(core)[3:]])
                far, new, (total,) = shared(
                    sides, a1, peer_a, dy[0], peer_dy, saved, weights, None, stacks, moments, new, steps, jobs
                )
            elif kind == "s":
                far = send(far, beside)
            elif kind == "t":
                total = send(total, beside)
            elif kind == "Z":
                both_sides = jnp.concatenate([table(core)[:3], table(1 - core)[3:]])
                far, new, _ = shared(both_sides, a1, peer_a, dy[0], peer_dy, saved, weights, far, [total], moments, new, steps, jobs)
            elif kind == "k":
                far_other = send(far, beside)
            elif kind in "CD":
                side, g = (core, far) if kind == "C" else (1 - core, far_other)
                new, _ = adamw(offset(side, NEAR), [g], weights, m, v, new, 1, 0)
            elif kind == "x":
                k = int(name[1:]) - NX
                pair[k][1] = send(pair[k][0], across)
            elif kind == "h":
                have[name[1:]] = send(have["A" + name[1:]], beside)
            else:
                ks = chunks_of(name)
                number, first = ks[0] - NEAR, str(ks[0])
                if kind == "A":
                    gs = [z for k in ks for z in pair[k - NX]]
                    new, (have["A" + first],) = adamw(offset(core, number), gs, weights, m, v, new, 0, 1)
                else:
                    new, _ = adamw(offset(1 - core, number), [have[first]], weights, m, v, new, 0, 0)
        return tuple(new)

    return jax.shard_map(
        step,
        mesh=mesh,
        in_specs=(P(("rep", "dp"), None, None),) * 2 + (P(None, None, None),) * 9,
        out_specs=(P("rep", None, None),) * 9,
        check_vma=False,
    )
```

```python
import functools

import jax
import jax.numpy as jnp
from jax import lax
from jax.experimental import pallas as pl
from jax.experimental.pallas import tpu as pltpu
from jax.sharding import PartitionSpec as P


BF, F32 = jnp.bfloat16, jnp.float32
AXES = ("rep", "dp")
MESH = pl.DeviceIdType.MESH
CHUNK = 512
ROWS = 512
ADAM_COLS = 256
ADAM_ROWS = 128
VMEM = 60 << 20
NEAR = 4
NX = 4


def sigmoid(x):
    return pl.reciprocal(1.0 + jnp.exp(-x), approx=False)


def nn(a, b):
    return jnp.dot(a, b, preferred_element_type=F32)


def nt(a, b):
    return lax.dot_general(a, b, (((1,), (1,)), ((), ())), preferred_element_type=F32)


def tn(a, b):
    return lax.dot_general(a, b, (((0,), (0,)), ((), ())), preferred_element_type=F32)


def scale_of(wide):
    return lax.rsqrt(jnp.mean(wide * wide, -1, keepdims=True) + 1e-6)


def normed(h):
    wide = h.astype(F32)
    return (wide * scale_of(wide)).astype(BF)


def forward_kernel(rows_, h_ref, wg_ref, wu_ref, wd_ref, out_ref, a_ref, next_ref, gate_ref, up_ref, acc_ref, p_s):
    step = pl.program_id(0)

    @pl.when(step == 0)
    def _():
        a_ref[...] = normed(h_ref[...])
        acc_ref[...] = jnp.zeros_like(acc_ref)

    for r in range(h_ref.shape[0] // rows_):
        rows = pl.ds(r * rows_, rows_)
        a = a_ref[rows]
        gate = nn(a, wg_ref[...])
        up = nn(a, wu_ref[...])
        gate_ref[rows] = gate
        up_ref[rows] = up
        p_s[rows] = (gate * sigmoid(gate) * up).astype(BF)
    for r in range(h_ref.shape[0] // rows_):
        rows = pl.ds(r * rows_, rows_)
        acc_ref[rows] += nn(p_s[rows], wd_ref[...])

    @pl.when(step == pl.num_programs(0) - 1)
    def _():
        h = h_ref[...] + acc_ref[...].astype(BF)
        out_ref[...] = h
        next_ref[...] = normed(h)


def forward(h, wg, wu, wd, layer, chunk=512, rows=512):
    t, d = h.shape
    ff = wg.shape[2]
    full = pl.BlockSpec((t, d), lambda j: (0, 0))
    wide = pl.BlockSpec((None, d, chunk), lambda j: (layer, 0, j))
    cols = pl.BlockSpec((None, t, chunk), lambda j: (j, 0, 0))
    return pl.pallas_call(
        functools.partial(forward_kernel, rows),
        grid=(ff // chunk,),
        in_specs=[full, wide, wide, pl.BlockSpec((None, chunk, d), lambda j: (layer, j, 0))],
        out_specs=[full] * 3 + [cols] * 2,
        out_shape=[jax.ShapeDtypeStruct((t, d), BF)] * 3 + [jax.ShapeDtypeStruct((ff // chunk, t, chunk), F32)] * 2,
        scratch_shapes=[pltpu.VMEM((t, d), F32), pltpu.VMEM((t, chunk), BF)],
        compiler_params=pltpu.CompilerParams(vmem_limit_bytes=VMEM),
        cost_estimate=pl.CostEstimate(flops=6 * t * d * ff, bytes_accessed=8 * t * ff, transcendentals=0),
        name="forward",
    )(h, wg, wu, wd)


def middle(gate, up, dp, rows, p_s, dg_s, du_s):
    dp = dp.astype(BF).astype(F32)
    s = sigmoid(gate)
    silu = gate * s
    p_s[rows] = (silu * up).astype(BF)
    du_s[rows] = (dp * silu).astype(BF)
    dg_s[rows] = (dp * up * (s + silu * (1.0 - s))).astype(BF)


def both_kernel(near, nx, a1, h1, dy, a0, wg, wu, wd, gate0, up0, *refs):
    per = wd.shape[1] // 2 // CHUNK
    far = per - near
    n = near + per
    refs = list(refs)
    take = lambda k: [refs.pop(0) for _ in range(k)]
    stacked, came, *sums = take(2 + n - nx)
    sums = [stacked.at[k] for k in range(nx)] + sums
    (landed,) = take(1)
    saved = take(3)
    (peer_a,) = take(1)
    a_v, dy_v, b_v, da_v, p_s, dg_s, du_s, wg_v, wu_v, wd_v, gate_v, up_v, add_v, grad_v = take(14)
    in_sem, w_sem, g_sem, add_sem, out_sem, save_sem, d_send, d_recv, x_send, x_recv, a_send, a_recv = take(12)
    t_save, t_low, steps = 2 * near, 2 * per, 4 * per
    j = pl.program_id(0)
    rep, dp = lax.axis_index("rep"), lax.axis_index("dp")
    core = lax.rem(dp, 2)
    beside = (rep, dp + 1 - 2 * core)
    across = (rep, lax.rem(dp + 2, 4))
    t = a_v.shape[0]

    def saving(j):
        return (j >= t_save) & (j < t_low)

    def what(j):
        low = j >= t_low
        m = jnp.where(low, per, near)
        k = jnp.where(low, j - t_low, j)
        own = ((k >= 2) & (lax.rem(k, 2) == 0)) | (k == 2 * m - 1)
        number = jnp.where(own, jnp.where(k == 2 * m - 1, m - 1, k // 2 - 1), (k + 1) // 2)
        return own & jnp.logical_not(saving(j)), number, jnp.where(low, near, 0) + number

    def gives(j, own):
        mine = what(j)[0]
        return (j < steps) & jnp.logical_not(saving(j)) & (mine if own else jnp.logical_not(mine))

    def block_of(j):
        own, number, _ = what(j)
        side = jnp.where(own, core, 1 - core)
        k = j - t_save
        near_block = side * per + number
        return jnp.where(saving(j), (k // far) * per + near + lax.rem(k, far), near_block) if far else near_block

    def loads(j, top):
        s = lax.rem(j, 2)
        block = block_of(j)
        cols = pl.ds(pl.multiple_of(block * CHUNK, CHUNK), CHUNK)
        if top:
            return [
                pltpu.make_async_copy(wg.at[1, :, cols], wg_v.at[s], w_sem.at[s, 0]),
                pltpu.make_async_copy(wu.at[1, :, cols], wu_v.at[s], w_sem.at[s, 1]),
                pltpu.make_async_copy(wd.at[1, cols], wd_v.at[s], w_sem.at[s, 2]),
            ]
        return [
            pltpu.make_async_copy(gate0.at[block], gate_v.at[s], g_sem.at[s, 0]),
            pltpu.make_async_copy(up0.at[block], up_v.at[s], g_sem.at[s, 1]),
            pltpu.make_async_copy(wd.at[0, cols], wd_v.at[s], w_sem.at[s, 2]),
        ]

    def load(j, do):
        @pl.when(j < t_low)
        def _():
            for c in loads(j, True):
                do(c)

        @pl.when((j >= t_low) & (j < steps))
        def _():
            for c in loads(j, False):
                do(c)

    start, wait = (lambda c: c.start()), (lambda c: c.wait())
    slot = lax.rem(j, 2)

    def d2d(q, s):
        return pltpu.make_async_remote_copy(
            src_ref=grad_v.at[s], dst_ref=landed.at[q], send_sem=d_send.at[q], recv_sem=d_recv.at[q], device_id=beside, device_id_type=MESH
        )

    def exchange(k):
        return pltpu.make_async_remote_copy(
            src_ref=sums[k], dst_ref=came.at[k], send_sem=x_send.at[k], recv_sem=x_recv.at[k], device_id=across, device_id_type=MESH
        )

    states = pltpu.make_async_remote_copy(
        src_ref=a1, dst_ref=peer_a, send_sem=a_send, recv_sem=a_recv, device_id=across, device_id_type=MESH
    )

    def add_copy(q, s):
        return pltpu.make_async_copy(landed.at[q], add_v.at[s], add_sem.at[s])

    def saves(j, s):
        return [pltpu.make_async_copy(z.at[s], out.at[j - t_save], save_sem.at[s, i]) for i, (z, out) in enumerate(zip((dg_s, du_s, p_s), saved))]

    def late(j):
        low = j >= t_low
        k = jnp.where(low, j - t_low, j)
        return (k == 2) | (k == jnp.where(low, t_low, t_save) - 1)

    def keep(j, do, k_max):
        q = what(j)[2]
        s = lax.rem(j, 2)
        for k in range(k_max):
            pl.when(gives(j, True) & (q == k))(lambda k=k: do(k, s))

    def kept(k, s):
        return pltpu.make_async_copy(grad_v.at[s], sums[k], out_sem.at[s])

    def ship(j):
        pl.when(gives(j, False))(lambda: d2d(what(j)[2], lax.rem(j, 2)).start())
        keep(j, lambda k, s: kept(k, s).start(), n)
        if far:

            @pl.when(saving(j))
            def _():
                for c in saves(j, lax.rem(j, 2)):
                    c.start()

    def settle(j):
        pl.when(gives(j, False))(lambda: d2d(what(j)[2], lax.rem(j, 2)).wait_send())

        def done(k, s):
            kept(k, s).wait()
            if k < nx:
                exchange(k).start()

        keep(j, done, n)
        if far:

            @pl.when(saving(j))
            def _():
                for c in saves(j, lax.rem(j, 2)):
                    c.wait()

    first_loads = [(a1, a_v), (dy, dy_v), (h1, b_v)]

    @pl.when(j == 0)
    def _():
        load(j, start)
        for k, (src, dst) in enumerate(first_loads):
            pltpu.make_async_copy(src, dst, in_sem.at[k]).start()
        barrier = pltpu.get_barrier_semaphore()
        for device in (beside, across):
            pl.semaphore_signal(barrier, inc=1, device_id=device, device_id_type=MESH)
        pl.semaphore_wait(barrier, 2)
        states.start()
        for k, (src, dst) in enumerate(first_loads):
            pltpu.make_async_copy(src, dst, in_sem.at[k]).wait()

    pl.when(j >= 2)(lambda: settle(j - 2))
    pl.when(j >= 1)(lambda: ship(j - 1))
    load(j, wait)
    load(j + 1, start)

    def fetch(j):
        q = what(j)[2]
        d2d(q, lax.rem(j, 2)).wait_recv()
        add_copy(q, lax.rem(j, 2)).start()

    pl.when(gives(j, True) & late(j))(lambda: fetch(j))
    pl.when(gives(j, True))(lambda: add_copy(what(j)[2], slot).wait())
    pl.when(gives(j + 1, True) & jnp.logical_not(late(j + 1)))(lambda: fetch(j + 1))

    @pl.when(gives(j, False))
    def _():
        add_v[slot] = jnp.zeros(add_v.shape[1:], BF)

    p_j, dg_j, du_j = p_s.at[slot], dg_s.at[slot], du_s.at[slot]

    def gradients():
        for k, (left, right) in enumerate(((a_v, dg_j), (a_v, du_j), (dy_v, p_j))):
            grad_v[slot, k] = (tn(left[...], right[...]) + add_v[slot, k].astype(F32)).astype(BF)

    def upper(grads):
        wgj, wuj, wdj = wg_v.at[slot], wu_v.at[slot], wd_v.at[slot]
        for r in range(t // ROWS):
            rows = pl.ds(r * ROWS, ROWS)
            a = a_v[rows]
            middle(nn(a, wgj[...]), nn(a, wuj[...]), nt(dy_v[rows], wdj[...]), rows, p_j, dg_j, du_j)
        if grads:
            gradients()
        for r in range(t // ROWS):
            rows = pl.ds(r * ROWS, ROWS)
            da_v[rows] = jnp.where(j == 0, 0.0, da_v[rows]) + (nt(dg_j[rows], wgj[...]) + nt(du_j[rows], wuj[...]))

    pl.when(j < t_save)(lambda: upper(True))
    if far:
        pl.when(saving(j))(lambda: upper(False))

    @pl.when(j == t_low - 1)
    def _():
        def turn(r, _):
            rows = pl.ds(pl.multiple_of(r * 256, 256), 256)
            wide = b_v[rows].astype(F32)
            da = da_v[rows].astype(BF).astype(F32)
            scale = scale_of(wide)
            dot = jnp.sum(da * wide, -1, keepdims=True)
            dwide = da * scale - wide * (scale * scale * scale * dot * (1.0 / wide.shape[-1]))
            dy_v[rows] = dy_v[rows] + dwide.astype(BF)
            return 0

        lax.fori_loop(0, t // 256, turn, 0)
        c = pltpu.make_async_copy(a0, a_v, in_sem.at[0])
        c.start()
        c.wait()

    @pl.when(j >= t_low)
    def _():
        gj, uj, wdj = gate_v.at[slot], up_v.at[slot], wd_v.at[slot]
        for r in range(t // ROWS):
            rows = pl.ds(r * ROWS, ROWS)
            middle(gj[rows], uj[rows], nt(dy_v[rows], wdj[...]), rows, p_j, dg_j, du_j)
        gradients()

    @pl.when(j == steps - 1)
    def _():
        ship(j)
        settle(j - 1)
        settle(j)
        for k in range(nx):
            exchange(k).wait()
        states.wait()


def both(a1, h1, dy, a0, weights, saved, near, nx):
    t, d = a1.shape
    ff = weights[2].shape[1]
    per = ff // 2 // CHUNK
    n = near + per
    anywhere = pl.BlockSpec(memory_space=pl.ANY)
    chunk = jax.ShapeDtypeStruct((3, d, CHUNK), BF)
    kept = jax.ShapeDtypeStruct((2 * (per - near), t, CHUNK), BF)
    stack = jax.ShapeDtypeStruct((nx, 3, d, CHUNK), BF)
    outs = [stack] * 2 + [chunk] * (n - nx) + [jax.ShapeDtypeStruct((n, 3, d, CHUNK), BF)] + [kept] * 3 + [jax.ShapeDtypeStruct((t, d), BF)]
    dma = pltpu.SemaphoreType.DMA
    out = pl.pallas_call(
        functools.partial(both_kernel, near, nx),
        grid=(4 * per,),
        in_specs=[anywhere] * 9,
        out_specs=[anywhere] * len(outs),
        out_shape=outs,
        scratch_shapes=[pltpu.VMEM((t, d), BF)] * 3
        + [pltpu.VMEM((t, d), F32)]
        + [pltpu.VMEM((2, t, CHUNK), BF)] * 3
        + [pltpu.VMEM((2, d, CHUNK), BF)] * 2
        + [pltpu.VMEM((2, CHUNK, d), BF)]
        + [pltpu.VMEM((2, t, CHUNK), F32)] * 2
        + [pltpu.VMEM((2, 3, d, CHUNK), BF)] * 2
        + [dma((3,)), dma((2, 3)), dma((2, 2)), dma((2,)), dma((2,)), dma((2, 3))]
        + [dma((n,))] * 2
        + [dma((nx,))] * 2
        + [dma, dma],
        compiler_params=pltpu.CompilerParams(vmem_limit_bytes=67_000_000, collective_id=1, has_side_effects=True),
        cost_estimate=pl.CostEstimate(flops=24 * t * d * ff, bytes_accessed=8 * t * ff, transcendentals=0),
        name="backward",
    )(a1, h1, dy, a0, *weights, *saved)
    return out[:2], [[z, None] for z in out[2 : 2 + n - nx]], out[3 + n - nx : 6 + n - nx], out[6 + n - nx]


def adamw_block(gs, w, m, v, new_w, new_m, new_v, sum_ref):
    for i in range(3):
        g = gs[0][i].astype(F32)
        if sum_ref is not None:
            total = (g + gs[1][i].astype(F32)).astype(BF)
            sum_ref[i] = total
            g = total.astype(F32)
        if i == 2:
            g = g.T
        mi = 0.9 * m[i][...] + 0.1 * g
        vi = 0.95 * v[i][...] + 0.05 * g * g
        wi = w[i][...].astype(F32)
        step = mi * lax.rsqrt(vi + 1e-8) + 0.1 * wi
        new_w[i][...] = (wi - 0.02 * step).astype(BF)
        new_m[i][...] = mi
        new_v[i][...] = vi


def shared_kernel(own, aliased, table_ref, a_own, a_peer, dy_own, dy_peer, dg, du, p, wg_ref, wu_ref, wd_ref, *refs):
    refs = list(refs)
    take = lambda k: [refs.pop(0) for _ in range(k)]
    add_ref = take(1)[0] if own else None
    gs = take(1 if own else 2)
    w, m, v = take(3), take(3), take(3)
    take(9 * aliased)
    (out_ref,) = take(1)
    new = take(3), take(3), take(3)
    sum_ref = None if own else take(1)[0]
    a_st, dy_st, dg_s, du_s, p_s, in_sem, save_sem = take(7)
    j, part = pl.program_id(0), pl.program_id(1)
    t = a_own.shape[0]
    width = wd_ref.shape[0]
    per = CHUNK // width
    here = table_ref[0, 0]
    mine = pl.multiple_of(here * t, t)
    theirs = pl.multiple_of((1 - here) * t, t)

    def saves():
        block = table_ref[2, j]
        cols = pl.ds(pl.multiple_of(lax.rem(block, per) * width, width), width)
        return [
            pltpu.make_async_copy(src.at[block // per, :, cols], dst.at[pl.ds(mine, t)], save_sem.at[i])
            for i, (src, dst) in enumerate(((dg, dg_s), (du, du_s), (p, p_s)))
        ]

    @pl.when((j == 0) & (part == 0))
    def _():
        copies = [
            pltpu.make_async_copy(src, dst.at[pl.ds(at, t)], in_sem.at[i])
            for i, (src, dst, at) in enumerate(((a_peer, a_st, theirs), (dy_peer, dy_st, theirs), (a_own, a_st, mine), (dy_own, dy_st, mine)))
        ]
        for c in copies:
            c.start()
        for c in copies:
            c.wait()

    @pl.when(part == 0)
    def _():
        for c in saves():
            c.start()
        for r in range(t // ROWS):
            rows = pl.ds(pl.multiple_of(theirs + r * ROWS, ROWS), ROWS)
            a = a_st[rows]
            middle(nn(a, wg_ref[...]), nn(a, wu_ref[...]), nt(dy_st[rows], wd_ref[...]), rows, p_s, dg_s, du_s)
        adamw_block(gs, w, m, v, *new, sum_ref)

    @pl.when(part == 1)
    def _():
        for c in saves():
            c.wait()
        for k, (left, right) in enumerate(((a_st, dg_s), (a_st, du_s), (dy_st, p_s))):
            g = tn(left[...], right[...])
            if own:
                g += add_ref[k].astype(F32)
            out_ref[k] = g.astype(BF)
        adamw_block(gs, w, m, v, *new, sum_ref)


def shared(table, a_own, a_peer, dy_own, dy_peer, saved, weights, add, gs, moments, new, steps, jobs):
    t, d = a_own.shape
    own = add is not None
    width = ADAM_COLS
    anywhere = pl.BlockSpec(memory_space=pl.ANY)
    wide = pl.BlockSpec((None, d, width), lambda j, p, c: (1, 0, c[1, j]))
    part = pl.BlockSpec((3, d, width), lambda j, p, c: (0, 0, j))

    def job(j, p):
        return jnp.minimum(2 * j + p, jobs - 1)

    stack = pl.BlockSpec((None, 3, d, width), lambda j, p, c: (c[5, job(j, p)], 0, 0, c[6, job(j, p)]))
    across = pl.BlockSpec((None, d, width), lambda j, p, c: (c[3, job(j, p)], 0, c[4, job(j, p)]))
    down = pl.BlockSpec((None, width, d), lambda j, p, c: (c[3, job(j, p)], c[4, job(j, p)], 0))
    kinds = [across, across, down] * 3
    arrays = (*weights, *moments)
    out = [jax.ShapeDtypeStruct((3, d, steps * width), BF)] + [jax.ShapeDtypeStruct(x.shape, x.dtype) for x in arrays]
    dma = pltpu.SemaphoreType.DMA
    before = 11 + own + len(gs) + 9
    out = pl.pallas_call(
        functools.partial(shared_kernel, own, new is not None),
        grid_spec=pltpu.PrefetchScalarGridSpec(
            num_scalar_prefetch=1,
            grid=(steps, 2),
            in_specs=[anywhere] * 7
            + [wide, wide, pl.BlockSpec((None, width, d), lambda j, p, c: (1, c[1, j], 0))]
            + [part] * own
            + [stack] * len(gs)
            + kinds
            + [anywhere] * (9 if new is not None else 0),
            out_specs=[part] + kinds + [stack] * (not own),
            scratch_shapes=[pltpu.VMEM((2 * t, d), BF)] * 2 + [pltpu.VMEM((2 * t, width), BF)] * 3 + [dma((4,)), dma((3,))],
        ),
        out_shape=out + [jax.ShapeDtypeStruct(gs[0].shape, BF)] * (not own),
        input_output_aliases={before + i: 1 + i for i in range(9)} if new is not None else {},
        compiler_params=pltpu.CompilerParams(vmem_limit_bytes=67_000_000),
        cost_estimate=pl.CostEstimate(flops=18 * t * d * width * steps, bytes_accessed=22 * 3 * d * width * jobs, transcendentals=0),
        name="shared_own" if own else "shared_other",
    )(table, a_own, a_peer, dy_own, dy_peer, *saved, *weights, *([add] if own else []), *gs, *arrays, *(new or ()))
    return out[0], out[1:10], out[10:]


def adamw_slices(gs, w, m, v, new_w, new_m, new_v, sum_ref):
    for i in range(3):
        for j in range(0, gs[0].shape[1], ADAM_ROWS):
            at = slice(j, j + ADAM_ROWS)
            g = gs[0][i, at].astype(F32)
            if sum_ref is not None:
                total = (g + gs[1][i, at].astype(F32)).astype(BF)
                sum_ref[i, at] = total
                g = total.astype(F32)
            to = (slice(None), at) if i == 2 else (at, slice(None))
            if i == 2:
                g = g.T
            mi = 0.9 * m[i][to] + 0.1 * g
            vi = 0.95 * v[i][to] + 0.05 * g * g
            wi = w[i][to].astype(F32)
            step = mi * lax.rsqrt(vi + 1e-8) + 0.1 * wi
            new_w[i][to] = (wi - 0.02 * step).astype(BF)
            new_m[i][to] = mi
            new_v[i][to] = vi


def adamw_kernel(own, aliased, chunks, off_ref, *refs):
    gs, refs = refs[: (1 + own) * chunks], refs[(1 + own) * chunks :]
    w, m, v = refs[0:3], refs[3:6], refs[6:9]
    refs = refs[9 + 9 * aliased :]
    new_w, new_m, new_v = refs[0:3], refs[3:6], refs[6:9]

    def work(g_refs):
        adamw_slices(g_refs, w, m, v, new_w, new_m, new_v, refs[9] if own else None)

    per = CHUNK // ADAM_COLS
    for k in range(chunks if own else 1):
        g_refs = gs[k * (1 + own) : (k + 1) * (1 + own)]
        if own and chunks > 1:
            pl.when(pl.program_id(0) // per == k)(functools.partial(work, g_refs))
        else:
            work(g_refs)


def adamw(off, gs, weights, m, v, new, layer, own):
    d = weights[0].shape[1]
    chunks = len(gs) // 2 if own else 1
    unit = chunks * gs[0].shape[2]
    per = CHUNK // ADAM_COLS
    wide = pl.BlockSpec((None, d, ADAM_COLS), lambda j, o: (layer, 0, o[0] + j))
    tall = pl.BlockSpec((None, ADAM_COLS, d), lambda j, o: (layer, o[0] + j, 0))
    grad = pl.BlockSpec((3, d, ADAM_COLS), lambda j, o: (0, 0, j))

    def part(k):
        return pl.BlockSpec((3, d, ADAM_COLS), lambda j, o: (0, 0, jnp.clip(j - k * per, 0, per - 1)))

    kinds = [wide, wide, tall] * 3
    shapes = [jax.ShapeDtypeStruct(x.shape, x.dtype) for x in (*weights, *m, *v)]
    out = pl.pallas_call(
        functools.partial(adamw_kernel, own, new is not None, chunks),
        grid_spec=pltpu.PrefetchScalarGridSpec(
            num_scalar_prefetch=1,
            grid=(unit // ADAM_COLS,),
            in_specs=([part(k // 2) for k in range(2 * chunks)] if own else [grad])
            + kinds
            + ([pl.BlockSpec(memory_space=pl.ANY)] * 9 if new is not None else []),
            out_specs=kinds + [grad] * own,
        ),
        out_shape=shapes + [jax.ShapeDtypeStruct((3, d, unit), BF)] * own,
        input_output_aliases={10 + len(gs) + i: i for i in range(9)} if new is not None else {},
        compiler_params=pltpu.CompilerParams(vmem_limit_bytes=VMEM),
        cost_estimate=pl.CostEstimate(flops=int(8 * 3 * d * unit * 30), bytes_accessed=22 * 3 * d * unit, transcendentals=0),
        name="adamw_own" if own else "adamw_other",
    )(off, *gs, *weights, *m, *v, *(new or ()))
    return out[:9], out[9:]


ORDER = (
    "p0", "F", "G", "x4", "x5", "Y0", "s0", "t0", "x6", "x7", "A4", "h4",
    "x8", "Z0", "k0", "x9", "A5", "h5", "q9", "B4", "C0", "B5", "D0", "A6+7",
    "h6", "A8", "h8", "B6+7", "B8", "r9", "A9", "E9",
)


def chunks_of(name):
    first, *more = name[1:].split("+")
    return range(int(first), 1 + int(more[0] if more else first))


def solution(mesh):
    reps, dps = mesh.shape["rep"], mesh.shape["dp"]

    def pairs(to):
        return [(r * dps + i, r * dps + to(i)) for r in range(reps) for i in range(dps)]

    across = pairs(lambda i: (i + 2) % dps)
    beside = pairs(lambda i: i ^ 1)

    def step(x, dy, *arrays):
        weights, m, v = (arrays[i : i + 3] for i in (0, 3, 6))
        core = lax.axis_index("dp") % 2
        half = weights[0].shape[2] // 2
        per = half // CHUNK
        have = {}
        new = None

        def offset(side, number):
            return ((side * half + number * CHUNK) // ADAM_COLS).astype(jnp.int32).reshape(1)

        def send(z, to):
            return lax.ppermute(z, AXES, to)

        def table(side):
            far, parts = per - NEAR, CHUNK // ADAM_COLS
            k = jnp.arange(far * parts, dtype=jnp.int32)
            i = jnp.arange(NX * parts, dtype=jnp.int32)
            chunk, layer = i // parts, (i // parts < NEAR).astype(jnp.int32)
            number = chunk - (1 - layer) * NEAR
            rows = [where, (side * per + NEAR) * parts + k, side * far * parts + k, layer, (side * per + number) * parts + i % parts, chunk, i % parts]
            width = max(far, NX) * parts
            return jnp.stack([jnp.pad(r.astype(jnp.int32), (0, width - r.shape[0])) for r in rows])

        where = (lax.axis_index("dp") // 2).astype(jnp.int32).reshape(1)
        moments = (*m, *v)
        steps, jobs = (per - NEAR) * (CHUNK // ADAM_COLS), NX * (CHUNK // ADAM_COLS)
        for name in ORDER:
            kind = name[0]
            if kind == "p":
                peer_dy = send(dy[0], across)
            elif kind == "F":
                h1, a0, a1, gate0, up0 = forward(x[0], *weights, 0)
            elif kind == "G":
                stacks, pair, saved, peer_a = both(a1, h1, dy[0], a0, weights, (gate0, up0), NEAR, NX)
            elif kind == "Y":
                sides = jnp.concatenate([table(1 - core)[:3], table(core)[3:]])
                far, new, (total,) = shared(
                    sides, a1, peer_a, dy[0], peer_dy, saved, weights, None, stacks, moments, new, steps, jobs
                )
            elif kind == "s":
                far = send(far, beside)
            elif kind == "t":
                total = send(total, beside)
            elif kind == "Z":
                both_sides = jnp.concatenate([table(core)[:3], table(1 - core)[3:]])
                far, new, _ = shared(both_sides, a1, peer_a, dy[0], peer_dy, saved, weights, far, [total], moments, new, steps, jobs)
            elif kind == "k":
                far_other = send(far, beside)
            elif kind in "CD":
                side, g = (core, far) if kind == "C" else (1 - core, far_other)
                new, _ = adamw(offset(side, NEAR), [g], weights, m, v, new, 1, 0)
            elif kind == "x":
                k = int(name[1:]) - NX
                pair[k][1] = send(pair[k][0], across)
            elif kind in "qr":
                have[name] = send(pair[int(name[1:]) - NX][kind == "r"], beside)
            elif kind == "E":
                k = int(name[1:])
                new, _ = adamw(offset(1 - core, k - NEAR), [have[f"q{k}"], have[f"r{k}"]], weights, m, v, new, 0, 1)
            elif kind == "h":
                have[name[1:]] = send(have["A" + name[1:]], beside)
            else:
                ks = chunks_of(name)
                number, first = ks[0] - NEAR, str(ks[0])
                if kind == "A":
                    gs = [z for k in ks for z in pair[k - NX]]
                    new, (have["A" + first],) = adamw(offset(core, number), gs, weights, m, v, new, 0, 1)
                else:
                    new, _ = adamw(offset(1 - core, number), [have[first]], weights, m, v, new, 0, 0)
        return tuple(new)

    return jax.shard_map(
        step,
        mesh=mesh,
        in_specs=(P(("rep", "dp"), None, None),) * 2 + (P(None, None, None),) * 9,
        out_specs=(P("rep", None, None),) * 9,
        check_vma=False,
    )
```

```python
import functools

import jax
import jax.numpy as jnp
from jax import lax
from jax.experimental import pallas as pl
from jax.experimental.pallas import tpu as pltpu
from jax.sharding import PartitionSpec as P


BF, F32 = jnp.bfloat16, jnp.float32
AXES = ("rep", "dp")
MESH = pl.DeviceIdType.MESH
CHUNK = 512
ROWS = 512
ADAM_COLS = 256
ADAM_ROWS = 128
VMEM = 60 << 20
NEAR = 4
NX = 4


def sigmoid(x):
    return pl.reciprocal(1.0 + jnp.exp(-x), approx=False)


def nn(a, b):
    return jnp.dot(a, b, preferred_element_type=F32)


def nt(a, b):
    return lax.dot_general(a, b, (((1,), (1,)), ((), ())), preferred_element_type=F32)


def tn(a, b):
    return lax.dot_general(a, b, (((0,), (0,)), ((), ())), preferred_element_type=F32)


def scale_of(wide):
    return lax.rsqrt(jnp.mean(wide * wide, -1, keepdims=True) + 1e-6)


def normed(h):
    wide = h.astype(F32)
    return (wide * scale_of(wide)).astype(BF)


def forward_kernel(rows_, h_ref, wg_ref, wu_ref, wd_ref, out_ref, a_ref, next_ref, gate_ref, up_ref, acc_ref, p_s):
    step = pl.program_id(0)

    @pl.when(step == 0)
    def _():
        a_ref[...] = normed(h_ref[...])
        acc_ref[...] = jnp.zeros_like(acc_ref)

    for r in range(h_ref.shape[0] // rows_):
        rows = pl.ds(r * rows_, rows_)
        a = a_ref[rows]
        gate = nn(a, wg_ref[...])
        up = nn(a, wu_ref[...])
        gate_ref[rows] = gate
        up_ref[rows] = up
        p_s[rows] = (gate * sigmoid(gate) * up).astype(BF)
    for r in range(h_ref.shape[0] // rows_):
        rows = pl.ds(r * rows_, rows_)
        acc_ref[rows] += nn(p_s[rows], wd_ref[...])

    @pl.when(step == pl.num_programs(0) - 1)
    def _():
        h = h_ref[...] + acc_ref[...].astype(BF)
        out_ref[...] = h
        next_ref[...] = normed(h)


def forward(h, wg, wu, wd, layer, chunk=512, rows=512):
    t, d = h.shape
    ff = wg.shape[2]
    full = pl.BlockSpec((t, d), lambda j: (0, 0))
    wide = pl.BlockSpec((None, d, chunk), lambda j: (layer, 0, j))
    cols = pl.BlockSpec((None, t, chunk), lambda j: (j, 0, 0))
    return pl.pallas_call(
        functools.partial(forward_kernel, rows),
        grid=(ff // chunk,),
        in_specs=[full, wide, wide, pl.BlockSpec((None, chunk, d), lambda j: (layer, j, 0))],
        out_specs=[full] * 3 + [cols] * 2,
        out_shape=[jax.ShapeDtypeStruct((t, d), BF)] * 3 + [jax.ShapeDtypeStruct((ff // chunk, t, chunk), F32)] * 2,
        scratch_shapes=[pltpu.VMEM((t, d), F32), pltpu.VMEM((t, chunk), BF)],
        compiler_params=pltpu.CompilerParams(vmem_limit_bytes=VMEM),
        cost_estimate=pl.CostEstimate(flops=6 * t * d * ff, bytes_accessed=8 * t * ff, transcendentals=0),
        name="forward",
    )(h, wg, wu, wd)


def middle(gate, up, dp, rows, p_s, dg_s, du_s):
    dp = dp.astype(BF).astype(F32)
    s = sigmoid(gate)
    silu = gate * s
    p_s[rows] = (silu * up).astype(BF)
    du_s[rows] = (dp * silu).astype(BF)
    dg_s[rows] = (dp * up * (s + silu * (1.0 - s))).astype(BF)


def both_kernel(near, nx, a1, h1, dy, a0, wg, wu, wd, gate0, up0, *refs):
    per = wd.shape[1] // 2 // CHUNK
    far = per - near
    n = near + per
    refs = list(refs)
    take = lambda k: [refs.pop(0) for _ in range(k)]
    stacked, came, *sums = take(2 + n - nx)
    sums = [stacked.at[k] for k in range(nx)] + sums
    (landed,) = take(1)
    saved = take(3)
    (peer_a,) = take(1)
    a_v, dy_v, b_v, da_v, p_s, dg_s, du_s, wg_v, wu_v, wd_v, gate_v, up_v, add_v, grad_v = take(14)
    in_sem, w_sem, g_sem, add_sem, out_sem, save_sem, d_send, d_recv, x_send, x_recv, a_send, a_recv = take(12)
    t_save, t_low, steps = 2 * near, 2 * per, 4 * per
    j = pl.program_id(0)
    rep, dp = lax.axis_index("rep"), lax.axis_index("dp")
    core = lax.rem(dp, 2)
    beside = (rep, dp + 1 - 2 * core)
    across = (rep, lax.rem(dp + 2, 4))
    t = a_v.shape[0]

    def saving(j):
        return (j >= t_save) & (j < t_low)

    def what(j):
        low = j >= t_low
        m = jnp.where(low, per, near)
        k = jnp.where(low, j - t_low, j)
        own = ((k >= 2) & (lax.rem(k, 2) == 0)) | (k == 2 * m - 1)
        number = jnp.where(own, jnp.where(k == 2 * m - 1, m - 1, k // 2 - 1), (k + 1) // 2)
        return own & jnp.logical_not(saving(j)), number, jnp.where(low, near, 0) + number

    def gives(j, own):
        mine = what(j)[0]
        return (j < steps) & jnp.logical_not(saving(j)) & (mine if own else jnp.logical_not(mine))

    def block_of(j):
        own, number, _ = what(j)
        side = jnp.where(own, core, 1 - core)
        k = j - t_save
        near_block = side * per + number
        return jnp.where(saving(j), (k // far) * per + near + lax.rem(k, far), near_block) if far else near_block

    def loads(j, top):
        s = lax.rem(j, 2)
        block = block_of(j)
        cols = pl.ds(pl.multiple_of(block * CHUNK, CHUNK), CHUNK)
        if top:
            return [
                pltpu.make_async_copy(wg.at[1, :, cols], wg_v.at[s], w_sem.at[s, 0]),
                pltpu.make_async_copy(wu.at[1, :, cols], wu_v.at[s], w_sem.at[s, 1]),
                pltpu.make_async_copy(wd.at[1, cols], wd_v.at[s], w_sem.at[s, 2]),
            ]
        return [
            pltpu.make_async_copy(gate0.at[block], gate_v.at[s], g_sem.at[s, 0]),
            pltpu.make_async_copy(up0.at[block], up_v.at[s], g_sem.at[s, 1]),
            pltpu.make_async_copy(wd.at[0, cols], wd_v.at[s], w_sem.at[s, 2]),
        ]

    def load(j, do):
        @pl.when(j < t_low)
        def _():
            for c in loads(j, True):
                do(c)

        @pl.when((j >= t_low) & (j < steps))
        def _():
            for c in loads(j, False):
                do(c)

    start, wait = (lambda c: c.start()), (lambda c: c.wait())
    slot = lax.rem(j, 2)

    def d2d(q, s):
        return pltpu.make_async_remote_copy(
            src_ref=grad_v.at[s], dst_ref=landed.at[q], send_sem=d_send.at[q], recv_sem=d_recv.at[q], device_id=beside, device_id_type=MESH
        )

    def exchange(k):
        return pltpu.make_async_remote_copy(
            src_ref=sums[k], dst_ref=came.at[k], send_sem=x_send.at[k], recv_sem=x_recv.at[k], device_id=across, device_id_type=MESH
        )

    states = pltpu.make_async_remote_copy(
        src_ref=a1, dst_ref=peer_a, send_sem=a_send, recv_sem=a_recv, device_id=across, device_id_type=MESH
    )

    def add_copy(q, s):
        return pltpu.make_async_copy(landed.at[q], add_v.at[s], add_sem.at[s])

    def saves(j, s):
        return [pltpu.make_async_copy(z.at[s], out.at[j - t_save], save_sem.at[s, i]) for i, (z, out) in enumerate(zip((dg_s, du_s, p_s), saved))]

    def late(j):
        low = j >= t_low
        k = jnp.where(low, j - t_low, j)
        return (k == 2) | (k == jnp.where(low, t_low, t_save) - 1)

    def keep(j, do, k_max):
        q = what(j)[2]
        s = lax.rem(j, 2)
        for k in range(k_max):
            pl.when(gives(j, True) & (q == k))(lambda k=k: do(k, s))

    def kept(k, s):
        return pltpu.make_async_copy(grad_v.at[s], sums[k], out_sem.at[s])

    def ship(j):
        pl.when(gives(j, False))(lambda: d2d(what(j)[2], lax.rem(j, 2)).start())
        keep(j, lambda k, s: kept(k, s).start(), n)
        if far:

            @pl.when(saving(j))
            def _():
                for c in saves(j, lax.rem(j, 2)):
                    c.start()

    def settle(j):
        pl.when(gives(j, False))(lambda: d2d(what(j)[2], lax.rem(j, 2)).wait_send())

        def done(k, s):
            kept(k, s).wait()
            if k < nx:
                exchange(k).start()

        keep(j, done, n)
        if far:

            @pl.when(saving(j))
            def _():
                for c in saves(j, lax.rem(j, 2)):
                    c.wait()

    first_loads = [(a1, a_v), (dy, dy_v), (h1, b_v)]

    @pl.when(j == 0)
    def _():
        load(j, start)
        for k, (src, dst) in enumerate(first_loads):
            pltpu.make_async_copy(src, dst, in_sem.at[k]).start()
        barrier = pltpu.get_barrier_semaphore()
        for device in (beside, across):
            pl.semaphore_signal(barrier, inc=1, device_id=device, device_id_type=MESH)
        pl.semaphore_wait(barrier, 2)
        states.start()
        for k, (src, dst) in enumerate(first_loads):
            pltpu.make_async_copy(src, dst, in_sem.at[k]).wait()

    pl.when(j >= 2)(lambda: settle(j - 2))
    pl.when(j >= 1)(lambda: ship(j - 1))
    load(j, wait)
    load(j + 1, start)

    def fetch(j):
        q = what(j)[2]
        d2d(q, lax.rem(j, 2)).wait_recv()
        add_copy(q, lax.rem(j, 2)).start()

    pl.when(gives(j, True) & late(j))(lambda: fetch(j))
    pl.when(gives(j, True))(lambda: add_copy(what(j)[2], slot).wait())
    pl.when(gives(j + 1, True) & jnp.logical_not(late(j + 1)))(lambda: fetch(j + 1))

    @pl.when(gives(j, False))
    def _():
        add_v[slot] = jnp.zeros(add_v.shape[1:], BF)

    p_j, dg_j, du_j = p_s.at[slot], dg_s.at[slot], du_s.at[slot]

    def gradients():
        for k, (left, right) in enumerate(((a_v, dg_j), (a_v, du_j), (dy_v, p_j))):
            grad_v[slot, k] = (tn(left[...], right[...]) + add_v[slot, k].astype(F32)).astype(BF)

    def upper(grads):
        wgj, wuj, wdj = wg_v.at[slot], wu_v.at[slot], wd_v.at[slot]
        for r in range(t // ROWS):
            rows = pl.ds(r * ROWS, ROWS)
            a = a_v[rows]
            middle(nn(a, wgj[...]), nn(a, wuj[...]), nt(dy_v[rows], wdj[...]), rows, p_j, dg_j, du_j)
        if grads:
            gradients()
        for r in range(t // ROWS):
            rows = pl.ds(r * ROWS, ROWS)
            da_v[rows] = jnp.where(j == 0, 0.0, da_v[rows]) + (nt(dg_j[rows], wgj[...]) + nt(du_j[rows], wuj[...]))

    pl.when(j < t_save)(lambda: upper(True))
    if far:
        pl.when(saving(j))(lambda: upper(False))

    @pl.when(j == t_low - 1)
    def _():
        def turn(r, _):
            rows = pl.ds(pl.multiple_of(r * 256, 256), 256)
            wide = b_v[rows].astype(F32)
            da = da_v[rows].astype(BF).astype(F32)
            scale = scale_of(wide)
            dot = jnp.sum(da * wide, -1, keepdims=True)
            dwide = da * scale - wide * (scale * scale * scale * dot * (1.0 / wide.shape[-1]))
            dy_v[rows] = dy_v[rows] + dwide.astype(BF)
            return 0

        lax.fori_loop(0, t // 256, turn, 0)
        c = pltpu.make_async_copy(a0, a_v, in_sem.at[0])
        c.start()
        c.wait()

    @pl.when(j >= t_low)
    def _():
        gj, uj, wdj = gate_v.at[slot], up_v.at[slot], wd_v.at[slot]
        for r in range(t // ROWS):
            rows = pl.ds(r * ROWS, ROWS)
            middle(gj[rows], uj[rows], nt(dy_v[rows], wdj[...]), rows, p_j, dg_j, du_j)
        gradients()

    @pl.when(j == steps - 1)
    def _():
        ship(j)
        settle(j - 1)
        settle(j)
        for k in range(nx):
            exchange(k).wait()
        states.wait()


def both(a1, h1, dy, a0, weights, saved, near, nx):
    t, d = a1.shape
    ff = weights[2].shape[1]
    per = ff // 2 // CHUNK
    n = near + per
    anywhere = pl.BlockSpec(memory_space=pl.ANY)
    chunk = jax.ShapeDtypeStruct((3, d, CHUNK), BF)
    kept = jax.ShapeDtypeStruct((2 * (per - near), t, CHUNK), BF)
    stack = jax.ShapeDtypeStruct((nx, 3, d, CHUNK), BF)
    outs = [stack] * 2 + [chunk] * (n - nx) + [jax.ShapeDtypeStruct((n, 3, d, CHUNK), BF)] + [kept] * 3 + [jax.ShapeDtypeStruct((t, d), BF)]
    dma = pltpu.SemaphoreType.DMA
    out = pl.pallas_call(
        functools.partial(both_kernel, near, nx),
        grid=(4 * per,),
        in_specs=[anywhere] * 9,
        out_specs=[anywhere] * len(outs),
        out_shape=outs,
        scratch_shapes=[pltpu.VMEM((t, d), BF)] * 3
        + [pltpu.VMEM((t, d), F32)]
        + [pltpu.VMEM((2, t, CHUNK), BF)] * 3
        + [pltpu.VMEM((2, d, CHUNK), BF)] * 2
        + [pltpu.VMEM((2, CHUNK, d), BF)]
        + [pltpu.VMEM((2, t, CHUNK), F32)] * 2
        + [pltpu.VMEM((2, 3, d, CHUNK), BF)] * 2
        + [dma((3,)), dma((2, 3)), dma((2, 2)), dma((2,)), dma((2,)), dma((2, 3))]
        + [dma((n,))] * 2
        + [dma((nx,))] * 2
        + [dma, dma],
        compiler_params=pltpu.CompilerParams(vmem_limit_bytes=67_000_000, collective_id=1, has_side_effects=True),
        cost_estimate=pl.CostEstimate(flops=24 * t * d * ff, bytes_accessed=8 * t * ff, transcendentals=0),
        name="backward",
    )(a1, h1, dy, a0, *weights, *saved)
    return out[:2], [[z, None] for z in out[2 : 2 + n - nx]], out[3 + n - nx : 6 + n - nx], out[6 + n - nx]


def adamw_block(gs, w, m, v, new_w, new_m, new_v, sum_ref):
    for i in range(3):
        g = gs[0][i].astype(F32)
        if sum_ref is not None:
            total = (g + gs[1][i].astype(F32)).astype(BF)
            sum_ref[i] = total
            g = total.astype(F32)
        if i == 2:
            g = g.T
        mi = 0.9 * m[i][...] + 0.1 * g
        vi = 0.95 * v[i][...] + 0.05 * g * g
        wi = w[i][...].astype(F32)
        step = mi * lax.rsqrt(vi + 1e-8) + 0.1 * wi
        new_w[i][...] = (wi - 0.02 * step).astype(BF)
        new_m[i][...] = mi
        new_v[i][...] = vi


def shared_kernel(own, aliased, table_ref, a_own, a_peer, dy_own, dy_peer, dg, du, p, wg_ref, wu_ref, wd_ref, *refs):
    refs = list(refs)
    take = lambda k: [refs.pop(0) for _ in range(k)]
    add_ref = take(1)[0] if own else None
    gs = take(1 if own else 2)
    w, m, v = take(3), take(3), take(3)
    take(9 * aliased)
    (out_ref,) = take(1)
    new = take(3), take(3), take(3)
    sum_ref = None if own else take(1)[0]
    a_st, dy_st, dg_s, du_s, p_s, in_sem, save_sem = take(7)
    j, part = pl.program_id(0), pl.program_id(1)
    t = a_own.shape[0]
    width = wd_ref.shape[0]
    per = CHUNK // width
    here = table_ref[0, 0]
    mine = pl.multiple_of(here * t, t)
    theirs = pl.multiple_of((1 - here) * t, t)

    def saves():
        block = table_ref[2, j]
        cols = pl.ds(pl.multiple_of(lax.rem(block, per) * width, width), width)
        return [
            pltpu.make_async_copy(src.at[block // per, :, cols], dst.at[pl.ds(mine, t)], save_sem.at[i])
            for i, (src, dst) in enumerate(((dg, dg_s), (du, du_s), (p, p_s)))
        ]

    @pl.when((j == 0) & (part == 0))
    def _():
        copies = [
            pltpu.make_async_copy(src, dst.at[pl.ds(at, t)], in_sem.at[i])
            for i, (src, dst, at) in enumerate(((a_peer, a_st, theirs), (dy_peer, dy_st, theirs), (a_own, a_st, mine), (dy_own, dy_st, mine)))
        ]
        for c in copies:
            c.start()
        for c in copies:
            c.wait()

    @pl.when(part == 0)
    def _():
        for c in saves():
            c.start()
        for r in range(t // ROWS):
            rows = pl.ds(pl.multiple_of(theirs + r * ROWS, ROWS), ROWS)
            a = a_st[rows]
            middle(nn(a, wg_ref[...]), nn(a, wu_ref[...]), nt(dy_st[rows], wd_ref[...]), rows, p_s, dg_s, du_s)
        adamw_block(gs, w, m, v, *new, sum_ref)

    @pl.when(part == 1)
    def _():
        for c in saves():
            c.wait()
        for k, (left, right) in enumerate(((a_st, dg_s), (a_st, du_s), (dy_st, p_s))):
            g = tn(left[...], right[...])
            if own:
                g += add_ref[k].astype(F32)
            out_ref[k] = g.astype(BF)
        adamw_block(gs, w, m, v, *new, sum_ref)


def shared(table, a_own, a_peer, dy_own, dy_peer, saved, weights, add, gs, moments, new, steps, jobs):
    t, d = a_own.shape
    own = add is not None
    width = ADAM_COLS
    anywhere = pl.BlockSpec(memory_space=pl.ANY)
    wide = pl.BlockSpec((None, d, width), lambda j, p, c: (1, 0, c[1, j]))
    part = pl.BlockSpec((3, d, width), lambda j, p, c: (0, 0, j))

    def job(j, p):
        return jnp.minimum(2 * j + p, jobs - 1)

    stack = pl.BlockSpec((None, 3, d, width), lambda j, p, c: (c[5, job(j, p)], 0, 0, c[6, job(j, p)]))
    across = pl.BlockSpec((None, d, width), lambda j, p, c: (c[3, job(j, p)], 0, c[4, job(j, p)]))
    down = pl.BlockSpec((None, width, d), lambda j, p, c: (c[3, job(j, p)], c[4, job(j, p)], 0))
    kinds = [across, across, down] * 3
    arrays = (*weights, *moments)
    out = [jax.ShapeDtypeStruct((3, d, steps * width), BF)] + [jax.ShapeDtypeStruct(x.shape, x.dtype) for x in arrays]
    dma = pltpu.SemaphoreType.DMA
    before = 11 + own + len(gs) + 9
    out = pl.pallas_call(
        functools.partial(shared_kernel, own, new is not None),
        grid_spec=pltpu.PrefetchScalarGridSpec(
            num_scalar_prefetch=1,
            grid=(steps, 2),
            in_specs=[anywhere] * 7
            + [wide, wide, pl.BlockSpec((None, width, d), lambda j, p, c: (1, c[1, j], 0))]
            + [part] * own
            + [stack] * len(gs)
            + kinds
            + [anywhere] * (9 if new is not None else 0),
            out_specs=[part] + kinds + [stack] * (not own),
            scratch_shapes=[pltpu.VMEM((2 * t, d), BF)] * 2 + [pltpu.VMEM((2 * t, width), BF)] * 3 + [dma((4,)), dma((3,))],
        ),
        out_shape=out + [jax.ShapeDtypeStruct(gs[0].shape, BF)] * (not own),
        input_output_aliases={before + i: 1 + i for i in range(9)} if new is not None else {},
        compiler_params=pltpu.CompilerParams(vmem_limit_bytes=67_000_000),
        cost_estimate=pl.CostEstimate(flops=18 * t * d * width * steps, bytes_accessed=22 * 3 * d * width * jobs, transcendentals=0),
        name="shared_own" if own else "shared_other",
    )(table, a_own, a_peer, dy_own, dy_peer, *saved, *weights, *([add] if own else []), *gs, *arrays, *(new or ()))
    return out[0], out[1:10], out[10:]


def adamw_slices(gs, w, m, v, new_w, new_m, new_v, sum_ref):
    for i in range(3):
        for j in range(0, gs[0].shape[1], ADAM_ROWS):
            at = slice(j, j + ADAM_ROWS)
            g = gs[0][i, at].astype(F32)
            if sum_ref is not None:
                total = (g + gs[1][i, at].astype(F32)).astype(BF)
                sum_ref[i, at] = total
                g = total.astype(F32)
            to = (slice(None), at) if i == 2 else (at, slice(None))
            if i == 2:
                g = g.T
            mi = 0.9 * m[i][to] + 0.1 * g
            vi = 0.95 * v[i][to] + 0.05 * g * g
            wi = w[i][to].astype(F32)
            step = mi * lax.rsqrt(vi + 1e-8) + 0.1 * wi
            new_w[i][to] = (wi - 0.02 * step).astype(BF)
            new_m[i][to] = mi
            new_v[i][to] = vi


def adamw_kernel(own, aliased, chunks, off_ref, *refs):
    gs, refs = refs[: (1 + own) * chunks], refs[(1 + own) * chunks :]
    w, m, v = refs[0:3], refs[3:6], refs[6:9]
    refs = refs[9 + 9 * aliased :]
    new_w, new_m, new_v = refs[0:3], refs[3:6], refs[6:9]

    def work(g_refs):
        adamw_slices(g_refs, w, m, v, new_w, new_m, new_v, refs[9] if own else None)

    per = CHUNK // ADAM_COLS
    for k in range(chunks if own else 1):
        g_refs = gs[k * (1 + own) : (k + 1) * (1 + own)]
        if own and chunks > 1:
            pl.when(pl.program_id(0) // per == k)(functools.partial(work, g_refs))
        else:
            work(g_refs)


def adamw(off, gs, weights, m, v, new, layer, own):
    d = weights[0].shape[1]
    chunks = len(gs) // 2 if own else 1
    unit = chunks * gs[0].shape[2]
    per = CHUNK // ADAM_COLS
    wide = pl.BlockSpec((None, d, ADAM_COLS), lambda j, o: (layer, 0, o[0] + j))
    tall = pl.BlockSpec((None, ADAM_COLS, d), lambda j, o: (layer, o[0] + j, 0))
    grad = pl.BlockSpec((3, d, ADAM_COLS), lambda j, o: (0, 0, j))

    def part(k):
        return pl.BlockSpec((3, d, ADAM_COLS), lambda j, o: (0, 0, jnp.clip(j - k * per, 0, per - 1)))

    kinds = [wide, wide, tall] * 3
    shapes = [jax.ShapeDtypeStruct(x.shape, x.dtype) for x in (*weights, *m, *v)]
    out = pl.pallas_call(
        functools.partial(adamw_kernel, own, new is not None, chunks),
        grid_spec=pltpu.PrefetchScalarGridSpec(
            num_scalar_prefetch=1,
            grid=(unit // ADAM_COLS,),
            in_specs=([part(k // 2) for k in range(2 * chunks)] if own else [grad])
            + kinds
            + ([pl.BlockSpec(memory_space=pl.ANY)] * 9 if new is not None else []),
            out_specs=kinds + [grad] * own,
        ),
        out_shape=shapes + [jax.ShapeDtypeStruct((3, d, unit), BF)] * own,
        input_output_aliases={10 + len(gs) + i: i for i in range(9)} if new is not None else {},
        compiler_params=pltpu.CompilerParams(vmem_limit_bytes=VMEM),
        cost_estimate=pl.CostEstimate(flops=int(8 * 3 * d * unit * 30), bytes_accessed=22 * 3 * d * unit, transcendentals=0),
        name="adamw_own" if own else "adamw_other",
    )(off, *gs, *weights, *m, *v, *(new or ()))
    return out[:9], out[9:]


ORDER = (
    "p0", "F", "G", "x4", "x5", "Y0", "s0", "t0", "x6", "x7", "A4", "h4",
    "x8", "Z0", "k0", "y0", "y1", "A5", "h5", "v0", "v1", "B4", "C0", "B5",
    "D0", "A6+7", "h6", "A8", "h8", "B6+7", "B8", "u0", "M0", "N0", "u1", "M1",
    "N1",
)


def chunks_of(name):
    first, *more = name[1:].split("+")
    return range(int(first), 1 + int(more[0] if more else first))


def solution(mesh):
    reps, dps = mesh.shape["rep"], mesh.shape["dp"]

    def pairs(to):
        return [(r * dps + i, r * dps + to(i)) for r in range(reps) for i in range(dps)]

    across = pairs(lambda i: (i + 2) % dps)
    beside = pairs(lambda i: i ^ 1)

    def step(x, dy, *arrays):
        weights, m, v = (arrays[i : i + 3] for i in (0, 3, 6))
        core = lax.axis_index("dp") % 2
        half = weights[0].shape[2] // 2
        per = half // CHUNK
        have = {}
        new = None

        def offset(side, number):
            return ((side * half + number * CHUNK) // ADAM_COLS).astype(jnp.int32).reshape(1)

        def send(z, to):
            return lax.ppermute(z, AXES, to)

        def table(side):
            far, parts = per - NEAR, CHUNK // ADAM_COLS
            k = jnp.arange(far * parts, dtype=jnp.int32)
            i = jnp.arange(NX * parts, dtype=jnp.int32)
            chunk, layer = i // parts, (i // parts < NEAR).astype(jnp.int32)
            number = chunk - (1 - layer) * NEAR
            rows = [where, (side * per + NEAR) * parts + k, side * far * parts + k, layer, (side * per + number) * parts + i % parts, chunk, i % parts]
            width = max(far, NX) * parts
            return jnp.stack([jnp.pad(r.astype(jnp.int32), (0, width - r.shape[0])) for r in rows])

        where = (lax.axis_index("dp") // 2).astype(jnp.int32).reshape(1)
        moments = (*m, *v)
        steps, jobs = (per - NEAR) * (CHUNK // ADAM_COLS), NX * (CHUNK // ADAM_COLS)
        for name in ORDER:
            kind = name[0]
            if kind == "p":
                peer_dy = send(dy[0], across)
            elif kind == "F":
                h1, a0, a1, gate0, up0 = forward(x[0], *weights, 0)
            elif kind == "G":
                stacks, pair, saved, peer_a = both(a1, h1, dy[0], a0, weights, (gate0, up0), NEAR, NX)
            elif kind == "Y":
                sides = jnp.concatenate([table(1 - core)[:3], table(core)[3:]])
                far, new, (total,) = shared(
                    sides, a1, peer_a, dy[0], peer_dy, saved, weights, None, stacks, moments, new, steps, jobs
                )
            elif kind == "s":
                far = send(far, beside)
            elif kind == "t":
                total = send(total, beside)
            elif kind == "Z":
                both_sides = jnp.concatenate([table(core)[:3], table(1 - core)[3:]])
                far, new, _ = shared(both_sides, a1, peer_a, dy[0], peer_dy, saved, weights, far, [total], moments, new, steps, jobs)
            elif kind == "k":
                far_other = send(far, beside)
            elif kind in "CD":
                side, g = (core, far) if kind == "C" else (1 - core, far_other)
                new, _ = adamw(offset(side, NEAR), [g], weights, m, v, new, 1, 0)
            elif kind == "x":
                k = int(name[1:]) - NX
                pair[k][1] = send(pair[k][0], across)
            elif kind in "yv":
                i = int(name[1:]) * ADAM_COLS
                have[name] = send(pair[-1][0][:, :, i : i + ADAM_COLS], across if kind == "y" else beside)
            elif kind == "u":
                have[name] = send(have["y" + name[1:]], beside)
            elif kind in "MN":
                i, side = int(name[1:]), core if kind == "M" else 1 - core
                mine = pair[-1][0][:, :, i * ADAM_COLS : (i + 1) * ADAM_COLS]
                gs = [mine, have[f"y{i}"]] if kind == "M" else [have[f"v{i}"], have[f"u{i}"]]
                new, _ = adamw(offset(side, per - 1) + i, gs, weights, m, v, new, 0, 1)
            elif kind == "h":
                have[name[1:]] = send(have["A" + name[1:]], beside)
            else:
                ks = chunks_of(name)
                number, first = ks[0] - NEAR, str(ks[0])
                if kind == "A":
                    gs = [z for k in ks for z in pair[k - NX]]
                    new, (have["A" + first],) = adamw(offset(core, number), gs, weights, m, v, new, 0, 1)
                else:
                    new, _ = adamw(offset(1 - core, number), [have[first]], weights, m, v, new, 0, 0)
        return tuple(new)

    return jax.shard_map(
        step,
        mesh=mesh,
        in_specs=(P(("rep", "dp"), None, None),) * 2 + (P(None, None, None),) * 9,
        out_specs=(P("rep", None, None),) * 9,
        check_vma=False,
    )
```
